512 devices in a mesh: sp: 4 (over x), bn: 8 (over z), dp: 16 (over y, core).
Axes of the slice: x: 4, y: 8, z: 8, core: 2. Of those that a mesh axis runs over, the one named last changes fastest.
Arguments:
- images: bfloat16 [128, 4, 64, 40, 128], P(('bn', 'dp'), 'sp'), may hold values from -8 to 8, as said below
- out_grad: bfloat16 [128, 4, 256, 40, 128], P(('bn', 'dp'), 'sp'), may hold values from -8 to 8, as said below
- conv_weight: bfloat16 [3, 3, 64, 64], replicated, may hold values from -0.25 to 0.25
- proj_weight: bfloat16 [64, 256], replicated, may hold values from -0.75 to 0.75
- gain_one: float32 [64], replicated, may hold values from 0.1 to 1.9
- shift_one: float32 [64], replicated, may hold values from -3 to 3
- gain_three: float32 [256], replicated, may hold values from 0.1 to 1.9
- shift_three: float32 [256], replicated, may hold values from -3 to 3
Outputs:
- images_grad: bfloat16 [128, 4, 64, 40, 128], P(('bn', 'dp'), 'sp')
- conv_grad: float32 [3, 3, 64, 64], replicated
- proj_grad: float32 [64, 256], replicated
- gain_one_grad: float32 [64], replicated
- shift_one_grad: float32 [64], replicated
- gain_three_grad: float32 [256], replicated
- shift_three_grad: float32 [256], replicated
The draws below stay inside these ranges and needn't reach their ends.
Inputs may be any that keep to these rules, and one draw needn't show every extreme that they name: `images`: channels of one quadrant have their own offset and spread. `out_grad`: channels of one quadrant have their own offset and spread.
All inputs are finite; a program needn't handle non-finite values.
Results may differ from the reference program's by a relative error of at most 0.029.
Values may be sent and summed in bfloat16 or wider, within the bound.
A program may use at most 64 MiB of HBM per device.

```python
import jax
import jax.numpy as jnp
from jax import lax

C = 64
CO = 256
TH = 40
TW = 128
IMG_DEV = 1
IMAGES = 128
N_BN = 8
N_DP = 16


def tile_draw(key, channels, salt_value):
    folded = jax.random.fold_in(key, salt_value)
    subkeys = jax.random.split(folded, 4)
    corner = (IMAGES, 4, channels, 1, 1)
    whole = (IMAGES, 4, channels, TH, TW)
    offsets = 1.5 * jax.random.normal(subkeys[0], corner, jnp.float32)
    spreads = jnp.exp(jax.random.uniform(subkeys[1], corner, jnp.float32, -1.2, 0.5))
    jitter = jax.random.normal(subkeys[2], whole, jnp.float32)
    drawn = offsets + spreads * jitter
    return jnp.clip(drawn, -8.0, 8.0)


def draw_images(key, part):
    return tile_draw(key, C, 3).astype(jnp.bfloat16)


def draw_out_grad(key, part):
    return tile_draw(key, CO, 7).astype(jnp.bfloat16)


def noise(stream_key, extent, scale, bound, held_as=jnp.bfloat16):
    return jnp.clip(scale * jax.random.normal(stream_key, extent, jnp.float32), -bound, bound).astype(held_as)


def setup_inputs(seed: int = 0) -> dict:
    key_of = jax.random.split(jax.random.key(seed), 9)
    return {
        "images": draw_images(jax.random.fold_in(key_of[8], 71), 0),
        "out_grad": draw_out_grad(jax.random.fold_in(key_of[8], 71), 0),
        "conv_weight": noise(key_of[2], (3, 3, C, C), (9 * C) ** -0.5, 0.25),
        "proj_weight": noise(key_of[3], (C, CO), C ** -0.5, 0.75),
        "gain_one": jnp.clip(1.0 + 0.18 * jax.random.normal(key_of[4], (C,), jnp.float32), 0.1, 1.9),
        "shift_one": noise(key_of[5], (C,), 1.0, 3.0, jnp.float32),
        "gain_three": jnp.clip(1.0 + 0.18 * jax.random.normal(key_of[6], (CO,), jnp.float32), 0.1, 1.9),
        "shift_three": noise(key_of[7], (CO,), 1.0, 3.0, jnp.float32),
    }


norm_floor = 1e-05

def silu_slope(inputs):
    sigma = jax.nn.sigmoid(inputs)
    return sigma * (1.0 + inputs * (1.0 - sigma))

def channel(vector):
    return vector[None, :, None, None]

def assemble(tiles):
    groups, quadrants, depth, tile_rows, tile_cols = tiles.shape
    merged = tiles.reshape(groups, 2, 2, depth, tile_rows, tile_cols)
    return merged.transpose(0, 3, 1, 4, 2, 5).reshape(groups, depth, 2 * tile_rows, 2 * tile_cols)

def split_back(field):
    groups, depth, height, breadth = field.shape
    parted = field.reshape(groups, depth, 2, height // 2, 2, breadth // 2)
    return parted.transpose(0, 2, 4, 1, 3, 5).reshape(groups, 4, depth, height // 2, breadth // 2)

def shifted(padded, start_row, start_col, height, breadth):
    return padded[:, :, start_row:start_row + height, start_col:start_col + breadth].astype(jnp.float32)

def pad_cells(field):
    return jnp.pad(field, ((0, 0), (0, 0), (1, 1), (1, 1)))

def moments(values):
    average = lax.optimization_barrier(jnp.mean(values, axis=(0, 2, 3)))
    centred = values - channel(average)
    return (average, lax.optimization_barrier(jnp.mean(centred * centred, axis=(0, 2, 3))))

def group_pass(image_tiles, cot_tiles, conv_weight, proj_weight, gain_one, shift_one, gain_three, shift_three):
    field = assemble(image_tiles)
    cotangent = assemble(cot_tiles)
    height = field.shape[2]
    breadth = field.shape[3]
    cell_count = field.shape[0] * height * breadth
    padded = pad_cells(field)
    kernel = conv_weight.astype(jnp.float32)
    conv_out = None
    for row_off in range(3):
        for col_off in range(3):
            partial_sum = jnp.einsum('oi,gihw->gohw', kernel[row_off, col_off], shifted(padded, row_off, col_off, height, breadth))
            conv_out = partial_sum if conv_out is None else conv_out + partial_sum
    mean_one, var_one = moments(conv_out)
    scale_one = lax.rsqrt(var_one + norm_floor)
    normed_one = (conv_out - channel(mean_one)) * channel(scale_one)
    before_act = channel(gain_one) * normed_one + channel(shift_one)
    hidden = jax.nn.silu(before_act).astype(jnp.bfloat16)
    hidden_float = hidden.astype(jnp.float32)
    project = proj_weight.astype(jnp.float32)
    widened = jnp.einsum('io,gihw->gohw', project, hidden_float)
    mean_three, var_three = moments(widened)
    scale_three = lax.rsqrt(var_three + norm_floor)
    normed_three = (widened - channel(mean_three)) * channel(scale_three)
    output_pre = channel(gain_three) * normed_three + channel(shift_three)
    grad_out = cotangent.astype(jnp.float32) * silu_slope(output_pre)
    sum_three = lax.optimization_barrier(jnp.sum(grad_out, axis=(0, 2, 3)))
    cross_three = lax.optimization_barrier(jnp.sum(grad_out * normed_three, axis=(0, 2, 3)))
    grad_wide = channel(gain_three * scale_three) * (grad_out - channel(sum_three) / cell_count - normed_three * channel(cross_three) / cell_count)
    grad_wide = grad_wide.astype(jnp.bfloat16).astype(jnp.float32)
    grad_proj = jnp.einsum('gihw,gohw->io', hidden_float, grad_wide)
    grad_hidden = jnp.einsum('io,gohw->gihw', project, grad_wide)
    grad_pre = grad_hidden * silu_slope(before_act)
    sum_one = lax.optimization_barrier(jnp.sum(grad_pre, axis=(0, 2, 3)))
    cross_one = lax.optimization_barrier(jnp.sum(grad_pre * normed_one, axis=(0, 2, 3)))
    grad_conv_out = channel(gain_one * scale_one) * (grad_pre - channel(sum_one) / cell_count - normed_one * channel(cross_one) / cell_count)
    grad_conv_out = grad_conv_out.astype(jnp.bfloat16)
    back_float = grad_conv_out.astype(jnp.float32)
    pieces_list = []
    for row_off in range(3):
        for col_off in range(3):
            pieces_list.append(jnp.einsum('gohw,gihw->oi', back_float, shifted(padded, row_off, col_off, height, breadth)))
    grad_kernel = jnp.stack(pieces_list).reshape(kernel.shape)
    back_pad = pad_cells(grad_conv_out)
    grad_field = None
    for row_off in range(3):
        for col_off in range(3):
            partial_sum = jnp.einsum('oi,gohw->gihw', kernel[row_off, col_off], shifted(back_pad, 2 - row_off, 2 - col_off, height, breadth))
            grad_field = partial_sum if grad_field is None else grad_field + partial_sum
    return (split_back(grad_field.astype(jnp.bfloat16)), grad_kernel, grad_proj, cross_one, sum_one, cross_three, sum_three)

def reference(images, out_grad, conv_weight, proj_weight, gain_one, shift_one, gain_three, shift_three):

    def regroup(tiles):
        depth = tiles.shape[2]
        sectioned = tiles.reshape(N_BN, N_DP, IMG_DEV, 4, depth, TH, TW).transpose(1, 0, 2, 3, 4, 5, 6)
        return sectioned.reshape(N_DP, N_BN * IMG_DEV, 4, depth, TH, TW)

    def one_group(inputs_pair):
        return group_pass(inputs_pair[0], inputs_pair[1], conv_weight, proj_weight, gain_one, shift_one, gain_three, shift_three)
    results = lax.map(one_group, (regroup(images), regroup(out_grad)))
    grad_tiles = results[0].reshape(N_DP, N_BN, IMG_DEV, 4, C, TH, TW).transpose(1, 0, 2, 3, 4, 5, 6)
    grad_tiles = grad_tiles.reshape(IMAGES, 4, C, TH, TW)
    per_image = 1.0 / (4 * TH * TW)
    return (grad_tiles, lax.optimization_barrier(jnp.sum(results[1], axis=0)) * per_image, lax.optimization_barrier(jnp.sum(results[2], axis=0)) * per_image, lax.optimization_barrier(jnp.sum(results[3], axis=0)) * per_image, lax.optimization_barrier(jnp.sum(results[4], axis=0)) * per_image, lax.optimization_barrier(jnp.sum(results[5], axis=0)) * per_image, lax.optimization_barrier(jnp.sum(results[6], axis=0)) * per_image)
```

```python
import functools

import jax
import jax.numpy as jnp
from jax import lax
from jax.experimental import pallas as pl
from jax.experimental.pallas import tpu as pltpu
from jax.sharding import PartitionSpec as P

MESH = pl.DeviceIdType.MESH
F32 = jnp.float32
BF16 = jnp.bfloat16
EPS = 1e-05
LANES = 128


def dot(a, b):
    return lax.dot_general(a, b, (((1,), (0,)), ((), ())), preferred_element_type=F32)


def dot_nt(a, b):
    return lax.dot_general(a, b, (((1,), (1,)), ((), ())), preferred_element_type=F32)


def to_column(row):
    return jnp.transpose(jnp.broadcast_to(row, (LANES, LANES)))


def columns_of(rows, depth):
    parts = [to_column(rows[k : k + 1]) for k in range(rows.shape[0])]
    return jnp.concatenate(parts, axis=0)[:depth] if len(parts) > 1 else parts[0][:depth]


def put_rows(ref, first, second):
    depth = first.shape[0]
    blocks = ref.shape[0] // 2
    lane = lax.broadcasted_iota(jnp.int32, (depth, LANES), 1)
    table = jnp.where(lane == 0, first, jnp.where(lane == 1, second, 0.0))
    if depth < LANES:
        table = jnp.concatenate([table, jnp.zeros((LANES - depth, LANES), F32)], axis=0)
    for k in range(blocks):
        turned = jnp.transpose(table[k * LANES : (k + 1) * LANES])
        ref[k : k + 1, :] = turned[0:1]
        ref[blocks + k : blocks + k + 1, :] = turned[1:2]


def kernel(
    n_sp, n_bn, n_dp, per_image,
    img, cot, cw, pw, g1, b1, g3, b3,
    o_img, o_cw, o_pw, o_g1, o_b1, o_g3, o_b3,
    xin, gin, flat, gflat, xs, hid, slope, ybuf, wide, egrad, das, out,
    wfwd, wbwd, wproj, col_s, col_r, row_r, diag_r, row_s, dcol_s, dcol_r, drow_s, drow_r, ddiag_r,
    m1s, m1r, m3s, m3r, q3s, q3r, q1s, q1r, dw, pg, tiles, rtiles, dts, dtr, vs, vr, ags, agr, vec,
    co3, co1, rsem, ssem, lsem,
):
    C, TH, W = xin.shape
    CO = gin.shape[0]
    NG = n_sp * n_bn
    nb1, nb3 = m1s.shape[0] // 2, m3s.shape[0] // 2
    n_local = float(TH * W)
    M = n_local * NG
    sp, bn, dp = lax.axis_index("sp"), lax.axis_index("bn"), lax.axis_index("dp")
    me = sp * n_bn + bn
    column = lax.rem(sp, 2)
    rowhalf = sp // 2

    def peer(k):
        return (lax.rem(sp + k // n_bn, n_sp), lax.rem(bn + lax.rem(k, n_bn), n_bn), dp)

    def across(k):
        return (sp, bn, lax.rem(dp + k, n_dp))

    in_x = pltpu.make_async_copy(img.at[0, 0], xin, lsem.at[0])
    in_g = pltpu.make_async_copy(cot.at[0, 0], gin, lsem.at[1])
    in_x.start()
    in_g.start()

    barrier = pltpu.get_barrier_semaphore()

    def greet(k, carry):
        pl.semaphore_signal(barrier, inc=1, device_id=peer(k), device_id_type=MESH)
        return carry

    lax.fori_loop(1, NG, greet, 0)

    def greet_across(k, carry):
        pl.semaphore_signal(barrier, inc=1, device_id=across(k), device_id_type=MESH)
        return carry

    lax.fori_loop(1, n_dp, greet_across, 0)

    taps = [cw[n // 3, n % 3].astype(F32) for n in range(9)]
    wfwd[...] = jnp.concatenate(taps, axis=1).astype(BF16)
    flipped = jnp.concatenate([taps[8 - n] for n in range(9)], axis=0)
    wbwd[...] = jnp.transpose(flipped).astype(BF16)
    wproj[...] = jnp.transpose(pw[...].astype(F32)).astype(BF16)
    vec[...] = jnp.zeros_like(vec)
    vec[0:1, 0:C] = g1[...]
    vec[1:2, 0:C] = b1[...]
    vec[2 : 2 + nb3, :] = g3[...]
    vec[2 + nb3 : 2 + 2 * nb3, :] = b3[...]

    in_x.wait()

    def widen(c, carry):
        flat[pl.ds(pl.multiple_of(c * TH, 8), TH), :] = xin[c].astype(F32)
        return carry

    lax.fori_loop(0, C, widen, 0, unroll=4)

    lane = lax.broadcasted_iota(jnp.int32, (C, W), 1)
    edge_mine = jnp.where(column == 0, W - 1, 0)
    edge_other = (W - 1) - edge_mine
    row_mine = jnp.where(rowhalf == 0, TH - 1, 0)
    halo_row = jnp.where(rowhalf == 0, TH + 1, 0)
    empty_row = (TH + 1) - halo_row

    def pick(h):
        return flat[pl.ds(h, C, stride=TH), :]

    def gather_column(row_of):
        def step(h, packed):
            turned = pltpu.roll(row_of(h), lax.rem(h - edge_mine + W, W), 1)
            return jnp.where(lane == h, turned, packed)

        return lax.fori_loop(0, TH, step, jnp.zeros((C, W), F32), unroll=4)

    col_s[...] = gather_column(pick).astype(BF16)
    row_s[...] = pick(row_mine).astype(BF16)

    pl.semaphore_wait(barrier, NG - 1 + n_dp - 1)

    beside = (sp + 1 - 2 * column, bn, dp)
    below = (lax.rem(sp + 2, 4), bn, dp)
    corner = (3 - sp, bn, dp)

    def halo(cs, cr, rs, rr, dr, base):
        return [
            pltpu.make_async_remote_copy(cs, cr, ssem.at[base], rsem.at[base], device_id=beside, device_id_type=MESH),
            pltpu.make_async_remote_copy(
                rs, rr, ssem.at[base + 1], rsem.at[base + 1], device_id=below, device_id_type=MESH
            ),
            pltpu.make_async_remote_copy(
                rs, dr, ssem.at[base + 2], rsem.at[base + 2], device_id=corner, device_id_type=MESH
            ),
        ]

    x_halo = halo(col_s, col_r, row_s, row_r, diag_r, 0)
    for copy in x_halo:
        copy.start()

    in_g.wait()

    def widen_g(c, carry):
        gflat[pl.ds(pl.multiple_of(c * TH, 8), TH), :] = gin[c].astype(F32)
        return carry

    lax.fori_loop(0, CO, widen_g, 0, unroll=8)

    def shifted_rows(dst, r, row, side):
        left = jnp.where(lane == 0, jnp.where(column == 1, side, 0.0), pltpu.roll(row, 1, 1))
        right = jnp.where(lane == W - 1, jnp.where(column == 0, side, 0.0), pltpu.roll(row, W - 1, 1))
        dst[r, 0:C, :] = left.astype(BF16)
        dst[r, C : 2 * C, :] = row.astype(BF16)
        dst[r, 2 * C : 3 * C, :] = right.astype(BF16)

    def build(dst, row_of, cr, rr, dr):
        sides = cr[...].astype(F32)

        def step(h, carry):
            shifted_rows(dst, h + 1, row_of(h), pltpu.roll(sides, lax.rem(edge_mine - h + W, W), 1))
            return carry

        lax.fori_loop(0, TH, step, 0, unroll=2)
        dst[empty_row] = jnp.zeros((3 * C, W), BF16)
        shifted_rows(dst, halo_row, rr[...].astype(F32), pltpu.roll(dr[...].astype(F32), lax.rem(edge_mine - edge_other + W, W), 1))

    for copy in x_halo:
        copy.wait()
    build(xs, pick, col_r, row_r, diag_r)

    R = 4

    def stack(src, h):
        parts = [src[pl.ds(h + j, 3)].reshape(9 * C, W) for j in range(R)]
        return jnp.concatenate(parts, axis=1)

    def conv(p, carry):
        h = p * R
        block = dot(wfwd[...], stack(xs, h))
        for j in range(R):
            hid[h + j] = block[:, j * W : (j + 1) * W]
        return carry

    lax.fori_loop(0, TH // R, conv, 0)

    def exchange(src, dst, n):
        pltpu.make_async_copy(src, dst.at[me], rsem.at[n]).start()

        def send(k, carry):
            pltpu.make_async_remote_copy(
                src, dst.at[me], ssem.at[n], rsem.at[n], device_id=peer(k), device_id_type=MESH
            ).start()
            return carry

        lax.fori_loop(1, NG, send, 0)

    def arrived(dst, n):
        pltpu.make_async_copy(dst, dst, rsem.at[n]).wait()

    def moments(src, depth, message):
        chunk = min(depth, 64)
        firsts, seconds = [], []
        for c in range(0, depth, chunk):
            base = jnp.sum(src[0, c : c + chunk, :], axis=1, keepdims=True) * (1.0 / W)
            shift = jnp.broadcast_to(base, (chunk, W))

            def step(p, carry):
                total, squares = carry
                for j in range(4):
                    v = src[p * 4 + j, c : c + chunk, :] - shift
                    total = total + v
                    squares = squares + v * v
                return total, squares

            zero = jnp.zeros((chunk, W), F32)
            total, squares = lax.fori_loop(0, TH // 4, step, (zero, zero))
            local = jnp.sum(total, axis=1, keepdims=True)
            firsts.append(base + local * (1.0 / n_local))
            seconds.append(jnp.sum(squares, axis=1, keepdims=True) - local * local * (1.0 / n_local))
        put_rows(message, jnp.concatenate(firsts, axis=0), jnp.concatenate(seconds, axis=0))

    def combined(ref, blocks):
        means = ref[:, 0:blocks, :]
        mean = jnp.sum(means, axis=0) * (1.0 / NG)
        off = means - mean[None]
        total = jnp.sum(ref[:, blocks : 2 * blocks, :], axis=0) + n_local * jnp.sum(off * off, axis=0)
        return mean, lax.rsqrt(total * (1.0 / M) + EPS)

    moments(hid, C, m1s)
    exchange(m1s, m1r, 6)
    arrived(m1r, 6)
    mean1, scale1 = combined(m1r, nb1)
    gain1, bias1 = vec[0:1, :], vec[1:2, :]
    co1[0] = columns_of(0.5 * gain1 * scale1, C)
    co1[1] = columns_of(0.5 * (bias1 - mean1 * gain1 * scale1), C)

    def activate(p, carry):
        h = p * R
        rows = []
        for j in range(R):
            half = hid[h + j] * co1[0] + co1[1]
            t = jnp.tanh(half)
            u = 1.0 + t
            y = (half * u).astype(BF16)
            hid[h + j] = half
            slope[h + j] = 0.5 * u * (1.0 + half * (1.0 - t))
            ybuf[h + j] = y
            rows.append(y)
        block = dot(wproj[...], jnp.concatenate(rows, axis=1))
        for j in range(R):
            wide[h + j] = block[:, j * W : (j + 1) * W]
        return carry

    lax.fori_loop(0, TH // R, activate, 0)

    moments(wide, CO, m3s)
    exchange(m3s, m3r, 7)
    arrived(m3r, 7)
    mean3, scale3 = combined(m3r, nb3)
    gain3, bias3 = vec[2 : 2 + nb3, :], vec[2 + nb3 : 2 + 2 * nb3, :]
    co3[0] = columns_of(0.5 * gain3 * scale3, CO)
    co3[1] = columns_of(0.5 * (bias3 - mean3 * gain3 * scale3), CO)

    step_c = 32
    firsts, seconds = [], []
    for c in range(0, CO, step_c):
        alpha, beta = co3[0, c : c + step_c, :], co3[1, c : c + step_c, :]

        def slopes(p, carry):
            total, cross = carry
            for j in range(4):
                h = p * 4 + j
                half = wide[h, c : c + step_c, :] * alpha + beta
                t = jnp.tanh(half)
                g = gflat[pl.ds(c * TH + h, step_c, stride=TH), :]
                e = g * ((1.0 + t) * (1.0 + half * (1.0 - t)))
                wide[h, c : c + step_c, :] = half
                egrad[h, c : c + step_c, :] = e
                total = total + e
                cross = cross + e * half
            return total, cross

        zero = jnp.zeros((step_c, W), F32)
        total, cross = lax.fori_loop(0, TH // 4, slopes, (zero, zero))
        firsts.append(jnp.sum(total, axis=1, keepdims=True))
        seconds.append(jnp.sum(cross, axis=1, keepdims=True))
    put_rows(q3s, jnp.concatenate(firsts, axis=0), jnp.concatenate(seconds, axis=0))
    exchange(q3s, q3r, 8)
    arrived(q3r, 8)
    e_sum = jnp.sum(q3r[:, 0:nb3, :], axis=0)
    eh_sum = jnp.sum(q3r[:, nb3 : 2 * nb3, :], axis=0)
    s3 = 0.5 * e_sum
    q3 = (eh_sum - bias3 * s3) / gain3
    vs[...] = jnp.zeros_like(vs)
    vs[0:nb3, :] = s3
    vs[nb3 : 2 * nb3, :] = q3
    co3[0] = columns_of(0.5 * gain3 * scale3, CO)
    co3[1] = columns_of((-2.0 / M) * scale3 * q3, CO)
    co3[2] = columns_of((1.0 / M) * scale3 * (q3 * bias3 - gain3 * s3), CO)

    pg[...] = jnp.zeros_like(pg)

    def unproject(p, carry):
        total, cross = carry
        h = p * R
        rows = []
        for j in range(R):
            pieces = []
            for c in range(0, CO, 64):
                part = slice(c, c + 64)
                grad = egrad[h + j, part, :] * co3[0, part, :] + wide[h + j, part, :] * co3[1, part, :]
                pieces.append((grad + co3[2, part, :]).astype(BF16))
            rows.append(jnp.concatenate(pieces, axis=0))
        grads = jnp.concatenate(rows, axis=1)
        hidden = jnp.concatenate([ybuf[h + j] for j in range(R)], axis=1)
        pg[...] += dot_nt(hidden, grads)
        block = dot(pw[...], grads)
        for j in range(R):
            e = block[:, j * W : (j + 1) * W] * slope[h + j]
            slope[h + j] = e
            total = total + e
            cross = cross + e * hid[h + j]
        return total, cross

    zero = jnp.zeros((C, W), F32)
    total, cross = lax.fori_loop(0, TH // R, unproject, (zero, zero))
    put_rows(q1s, jnp.sum(total, axis=1, keepdims=True), jnp.sum(cross, axis=1, keepdims=True))
    exchange(q1s, q1r, 9)

    lt_c = dw.shape[1] // LANES
    lt_p = CO // LANES
    n_conv = C // 16 * lt_c
    n_tiles = n_conv + C // 16 * lt_p

    def scatter(low, high):
        def send(k, carry):
            to = peer(k)
            owner = to[0] * n_bn + to[1]

            @pl.when(jnp.logical_and(owner >= low, owner < high))
            def _():
                pltpu.make_async_remote_copy(
                    tiles.at[owner], rtiles.at[me], ssem.at[10], rsem.at[10], device_id=to, device_id_type=MESH
                ).start()

            return carry

        @pl.when(jnp.logical_and(me >= low, me < high))
        def _():
            pltpu.make_async_copy(tiles.at[me], rtiles.at[me], rsem.at[10]).start()

        lax.fori_loop(1, NG, send, 0)

    for r in range(C // 16):
        for t in range(lt_p):
            tiles[n_conv + r * lt_p + t] = pg[r * 16 : (r + 1) * 16, t * LANES : (t + 1) * LANES].astype(BF16)
    scatter(n_conv, n_tiles)

    arrived(q1r, 9)
    s1 = jnp.sum(q1r[:, 0:nb1, :], axis=0)
    eh1 = jnp.sum(q1r[:, nb1 : 2 * nb1, :], axis=0)
    safe = jnp.where(lax.broadcasted_iota(jnp.int32, (1, LANES), 1) < C, gain1, 1.0)
    q1 = (2.0 * eh1 - bias1 * s1) / safe
    vs[2 * nb3 : 2 * nb3 + 1, :] = s1
    vs[2 * nb3 + 1 : 2 * nb3 + 2, :] = q1
    co1[0] = columns_of(gain1 * scale1, C)
    co1[1] = columns_of((-2.0 / M) * scale1 * q1, C)
    co1[2] = columns_of((1.0 / M) * scale1 * (q1 * bias1 - gain1 * s1), C)

    def spread(src, dst, n):
        pltpu.make_async_copy(src, dst.at[dp], rsem.at[n]).start()

        def send(k, carry):
            pltpu.make_async_remote_copy(
                src, dst.at[dp], ssem.at[n], rsem.at[n], device_id=across(k), device_id_type=MESH
            ).start()
            return carry

        lax.fori_loop(1, n_dp, send, 0)

    spread(vs, vr, 11)

    def unnorm(h, packed):
        row = slope[h] * co1[0] + hid[h] * co1[1] + co1[2]
        slope[h] = row
        das[h + 1, C : 2 * C, :] = row.astype(BF16)
        turned = pltpu.roll(row, lax.rem(h - edge_mine + W, W), 1)
        return jnp.where(lane == h, turned, packed)

    dcol_s[...] = lax.fori_loop(0, TH, unnorm, jnp.zeros((C, W), F32), unroll=4).astype(BF16)
    drow_s[...] = slope[row_mine].astype(BF16)
    d_halo = halo(dcol_s, dcol_r, drow_s, drow_r, ddiag_r, 3)
    for copy in d_halo:
        copy.start()

    dw[...] = jnp.zeros_like(dw)

    def weigh(p, carry):
        h = p * R
        grads = jnp.concatenate([das[h + j + 1, C : 2 * C, :] for j in range(R)], axis=1)
        dw[:, 0 : 9 * C] += dot_nt(grads, stack(xs, h))
        return carry

    lax.fori_loop(0, TH // R, weigh, 0)
    for r in range(C // 16):
        for t in range(lt_c):
            tiles[r * lt_c + t] = dw[r * 16 : (r + 1) * 16, t * LANES : (t + 1) * LANES].astype(BF16)
    scatter(0, n_conv)

    for copy in d_halo:
        copy.wait()
    build(das, lambda h: slope[h], dcol_r, drow_r, ddiag_r)

    def unconv(p, carry):
        h = p * R
        block = dot(wbwd[...], stack(das, h))
        for j in range(R):
            flat[pl.ds(h + j, C, stride=TH), :] = block[:, j * W : (j + 1) * W]
        return carry

    lax.fori_loop(0, TH // R, unconv, 0)

    @pl.when(me < n_tiles)
    def _():
        arrived(rtiles, 10)
        dts[...] = jnp.sum(rtiles[...].astype(F32), axis=0).astype(BF16)
        spread(dts, dtr, 12)

    def narrow(c, carry):
        out[c] = flat[pl.ds(pl.multiple_of(c * TH, 8), TH), :].astype(BF16)
        return carry

    lax.fori_loop(0, C, narrow, 0, unroll=4)
    put = pltpu.make_async_copy(out, o_img.at[0, 0], lsem.at[2])
    put.start()

    @pl.when(me < n_tiles)
    def _():
        arrived(dtr, 12)
        ags[...] = (jnp.sum(dtr[...].astype(F32), axis=0) * per_image).astype(BF16)
        exchange(ags, agr, 13)

    arrived(vr, 11)
    sums = jnp.sum(vr[...], axis=0) * per_image
    o_b3[...] = sums[0:nb3]
    o_g3[...] = sums[nb3 : 2 * nb3]
    o_b1[...] = sums[2 * nb3 : 2 * nb3 + 1, 0:C]
    o_g1[...] = sums[2 * nb3 + 1 : 2 * nb3 + 2, 0:C]

    gathered = agr.at[pl.ds(0, n_tiles)]
    pltpu.make_async_copy(gathered, gathered, rsem.at[13]).wait()
    for r in range(C // 16):
        rows = slice(r * 16, (r + 1) * 16)
        for t in range(lt_p):
            o_pw[rows, t * LANES : (t + 1) * LANES] = agr[n_conv + r * lt_p + t].astype(F32)
        line = [agr[r * lt_c + t].astype(F32) for t in range(lt_c)]
        line = jnp.concatenate(line, axis=1)
        for n in range(9):
            o_cw[n // 3, n % 3, rows, :] = line[:, n * C : (n + 1) * C]

    for dst, n in ((m1r, 6), (m3r, 7), (q3r, 8), (q1r, 9)):
        sent = dst.at[pl.ds(0, NG - 1)]
        pltpu.make_async_copy(sent, sent, ssem.at[n]).wait()
    sent = vr.at[pl.ds(0, n_dp - 1)]
    pltpu.make_async_copy(sent, sent, ssem.at[11]).wait()

    @pl.when(me < n_tiles)
    def _():
        sent = tiles.at[pl.ds(0, n_tiles - 1)]
        pltpu.make_async_copy(sent, sent, ssem.at[10]).wait()
        sent = dtr.at[pl.ds(0, n_dp - 1)]
        pltpu.make_async_copy(sent, sent, ssem.at[12]).wait()
        sent = agr.at[pl.ds(0, NG - 1)]
        pltpu.make_async_copy(sent, sent, ssem.at[13]).wait()

    @pl.when(me >= n_tiles)
    def _():
        sent = tiles.at[pl.ds(0, n_tiles)]
        pltpu.make_async_copy(sent, sent, ssem.at[10]).wait()

    put.wait()


def solution(mesh):
    n_sp, n_bn, n_dp = mesh.shape["sp"], mesh.shape["bn"], mesh.shape["dp"]
    NG = n_sp * n_bn

    def step(images, out_grad, conv_weight, proj_weight, gain_one, shift_one, gain_three, shift_three):
        C, TH, W = images.shape[2:]
        CO = out_grad.shape[2]
        nb1, nb3 = 1, CO // LANES
        wide_c = -(-9 * C // LANES) * LANES
        n_tiles = C // 16 * (wide_c // LANES + CO // LANES)
        vm = pltpu.VMEM
        scratch = [
            vm((C, TH, W), BF16), vm((CO, TH, W), BF16), vm((C * TH, W), F32), vm((CO * TH, W), F32),
            vm((TH + 2, 3 * C, W), BF16), vm((TH, C, W), F32), vm((TH, C, W), F32), vm((TH, C, W), BF16),
            vm((TH, CO, W), F32), vm((TH, CO, W), F32), vm((TH + 2, 3 * C, W), BF16), vm((C, TH, W), BF16),
            vm((C, 9 * C), BF16), vm((C, 9 * C), BF16), vm((CO, C), BF16),
            *[vm((C, W), BF16) for _ in range(10)][:5], *[vm((C, W), BF16) for _ in range(5)],
            vm((2 * nb1, LANES), F32), vm((NG, 2 * nb1, LANES), F32),
            vm((2 * nb3, LANES), F32), vm((NG, 2 * nb3, LANES), F32),
            vm((2 * nb3, LANES), F32), vm((NG, 2 * nb3, LANES), F32),
            vm((2 * nb1, LANES), F32), vm((NG, 2 * nb1, LANES), F32),
            vm((C, wide_c), F32), vm((C, CO), F32), vm((n_tiles, 16, LANES), BF16), vm((NG, 16, LANES), BF16),
            vm((16, LANES), BF16), vm((n_dp, 16, LANES), BF16), vm((8, LANES), F32), vm((n_dp, 8, LANES), F32),
            vm((16, LANES), BF16), vm((NG, 16, LANES), BF16), vm((8, LANES), F32),
            vm((3, CO, W), F32), vm((3, C, W), F32),
            pltpu.SemaphoreType.DMA((14,)), pltpu.SemaphoreType.DMA((14,)), pltpu.SemaphoreType.DMA((3,)),
        ]
        vspec = pl.BlockSpec(memory_space=pltpu.VMEM)
        aspec = pl.BlockSpec(memory_space=pl.ANY)
        shape = jax.ShapeDtypeStruct
        got = pl.pallas_call(
            functools.partial(kernel, n_sp, n_bn, n_dp, 1.0 / float(n_sp * TH * W)),
            out_shape=(
                shape(images.shape, BF16), shape((3, 3, C, C), F32), shape((C, CO), F32), shape((1, C), F32),
                shape((1, C), F32), shape((nb3, LANES), F32), shape((nb3, LANES), F32),
            ),
            in_specs=[aspec, aspec] + [vspec] * 6,
            out_specs=(aspec,) + (vspec,) * 6,
            scratch_shapes=scratch,
            compiler_params=pltpu.CompilerParams(
                collective_id=0, has_side_effects=True, vmem_limit_bytes=60 * 1024 * 1024
            ),
        )(
            images, out_grad, conv_weight, proj_weight, gain_one.reshape(1, C), shift_one.reshape(1, C),
            gain_three.reshape(nb3, LANES), shift_three.reshape(nb3, LANES),
        )
        return (
            got[0], got[1], got[2], got[3].reshape(C), got[4].reshape(C), got[5].reshape(CO), got[6].reshape(CO),
        )

    split = P(("bn", "dp"), "sp", None, None, None)
    return jax.shard_map(
        step,
        mesh=mesh,
        in_specs=(split, split) + (P(),) * 6,
        out_specs=(split,) + (P(),) * 6,
        check_vma=False,
    )
```

```python
import functools

import jax
import jax.numpy as jnp
from jax import lax
from jax.experimental import pallas as pl
from jax.experimental.pallas import tpu as pltpu
from jax.sharding import PartitionSpec as P

MESH = pl.DeviceIdType.MESH
F32 = jnp.float32
BF16 = jnp.bfloat16
EPS = 1e-05
LANES = 128


def dot(a, b):
    return lax.dot_general(a, b, (((1,), (0,)), ((), ())), preferred_element_type=F32)


def dot_nt(a, b):
    return lax.dot_general(a, b, (((1,), (1,)), ((), ())), preferred_element_type=F32)


def to_column(row):
    return jnp.transpose(jnp.broadcast_to(row, (LANES, LANES)))


def columns_of(rows, depth):
    parts = [to_column(rows[k : k + 1]) for k in range(rows.shape[0])]
    return jnp.concatenate(parts, axis=0)[:depth] if len(parts) > 1 else parts[0][:depth]


def put_rows(ref, first, second):
    depth = first.shape[0]
    blocks = ref.shape[0] // 2
    lane = lax.broadcasted_iota(jnp.int32, (depth, LANES), 1)
    table = jnp.where(lane == 0, first, jnp.where(lane == 1, second, 0.0))
    if depth < LANES:
        table = jnp.concatenate([table, jnp.zeros((LANES - depth, LANES), F32)], axis=0)
    for k in range(blocks):
        turned = jnp.transpose(table[k * LANES : (k + 1) * LANES])
        ref[k : k + 1, :] = turned[0:1]
        ref[blocks + k : blocks + k + 1, :] = turned[1:2]


def kernel(
    n_sp, n_bn, n_dp, per_image,
    img, cot, cw, pw, g1, b1, g3, b3,
    o_img, o_agr, o_sums,
    xin, gin, flat, gflat, xs, hid, slope, ybuf, wide, egrad, das, out,
    wfwd, wbwd, wproj, col_s, col_r, row_r, diag_r, row_s, dcol_s, dcol_r, drow_s, drow_r, ddiag_r,
    m1s, m1r, m3s, m3r, q3s, q3r, q1s, q1r, dw, pg, tiles, rtiles, dts, dtr, vs, vr, ags, agr, vec,
    co3, co1, dh, htiles, rhtiles, rsem, ssem, lsem,
):
    C, TH, W = xin.shape
    CO = gin.shape[0]
    NG = n_sp * n_bn
    nb1, nb3 = m1s.shape[0] // 2, m3s.shape[0] // 2
    n_local = float(TH * W)
    M = n_local * NG
    sp, bn, dp = lax.axis_index("sp"), lax.axis_index("bn"), lax.axis_index("dp")
    me = sp * n_bn + bn
    column = lax.rem(sp, 2)
    rowhalf = sp // 2

    def wrapped(at, step, size):
        moved = at + step
        return jnp.where(moved >= size, moved - size, moved)

    xs_of = [wrapped(sp, k, n_sp) for k in range(n_sp)]
    zs_of = [wrapped(bn, k, n_bn) for k in range(n_bn)]
    ds_of = [wrapped(dp, k, n_dp) for k in range(n_dp)]

    def ring(step, size):
        return min(step, size - step)

    peers = sorted(range(1, NG), key=lambda k: -ring(k // n_bn, n_sp) - ring(k % n_bn, n_bn))
    others = sorted(range(1, n_dp), key=lambda k: -ring(k // 2, n_dp // 2))

    def peer(k):
        return (xs_of[k // n_bn], zs_of[k % n_bn], dp)

    def across(k):
        return (sp, bn, ds_of[k])

    in_x = pltpu.make_async_copy(img.at[0, 0], xin, lsem.at[0])
    in_g = pltpu.make_async_copy(cot.at[0, 0], gin, lsem.at[1])
    in_x.start()
    in_g.start()

    barrier = pltpu.get_barrier_semaphore()

    for k in peers:
        pl.semaphore_signal(barrier, inc=1, device_id=peer(k), device_id_type=MESH)
    for k in others:
        pl.semaphore_signal(barrier, inc=1, device_id=across(k), device_id_type=MESH)

    taps = [cw[n // 3, n % 3].astype(F32) for n in range(9)]
    wfwd[...] = jnp.concatenate(taps, axis=1).astype(BF16)
    flipped = jnp.concatenate([taps[8 - n] for n in range(9)], axis=0)
    wbwd[...] = jnp.transpose(flipped).astype(BF16)
    wproj[...] = jnp.transpose(pw[...].astype(F32)).astype(BF16)
    vec[...] = jnp.zeros_like(vec)
    vec[0:1, 0:C] = g1[...]
    vec[1:2, 0:C] = b1[...]
    vec[2 : 2 + nb3, :] = g3[...]
    vec[2 + nb3 : 2 + 2 * nb3, :] = b3[...]

    in_x.wait()

    def widen(c, carry):
        flat[pl.ds(pl.multiple_of(c * TH, 8), TH), :] = xin[c].astype(F32)
        return carry

    lax.fori_loop(0, C, widen, 0, unroll=4)

    lane = lax.broadcasted_iota(jnp.int32, (C, W), 1)
    edge_mine = jnp.where(column == 0, W - 1, 0)
    edge_other = (W - 1) - edge_mine
    row_mine = jnp.where(rowhalf == 0, TH - 1, 0)
    halo_row = jnp.where(rowhalf == 0, TH + 1, 0)
    empty_row = (TH + 1) - halo_row

    def pick(h):
        return flat[pl.ds(h, C, stride=TH), :]

    def gather_column(row_of):
        def step(h, packed):
            turned = pltpu.roll(row_of(h), lax.rem(h - edge_mine + W, W), 1)
            return jnp.where(lane == h, turned, packed)

        return lax.fori_loop(0, TH, step, jnp.zeros((C, W), F32), unroll=4)

    col_s[...] = gather_column(pick).astype(BF16)
    row_s[...] = pick(row_mine).astype(BF16)

    def build(dst, h, row):
        left = jnp.where(lane == 0, 0.0, pltpu.roll(row, 1, 1))
        right = jnp.where(lane == W - 1, 0.0, pltpu.roll(row, W - 1, 1))
        dst[h + 1, 0:C, :] = left.astype(BF16)
        dst[h + 1, C : 2 * C, :] = row.astype(BF16)
        dst[h + 1, 2 * C : 3 * C, :] = right.astype(BF16)

    def lay_out(h, carry):
        build(xs, h, pick(h))
        return carry

    lax.fori_loop(0, TH, lay_out, 0, unroll=4)
    xs[empty_row] = jnp.zeros((3 * C, W), BF16)

    pl.semaphore_wait(barrier, NG - 1 + n_dp - 1)

    beside = (sp + 1 - 2 * column, bn, dp)
    below = (lax.rem(sp + 2, 4), bn, dp)
    corner = (3 - sp, bn, dp)

    def halo(cs, cr, rs, rr, dr, base):
        return [
            pltpu.make_async_remote_copy(cs, cr, ssem.at[base], rsem.at[base], device_id=beside, device_id_type=MESH),
            pltpu.make_async_remote_copy(
                rs, rr, ssem.at[base + 1], rsem.at[base + 1], device_id=below, device_id_type=MESH
            ),
            pltpu.make_async_remote_copy(
                rs, dr, ssem.at[base + 2], rsem.at[base + 2], device_id=corner, device_id_type=MESH
            ),
        ]

    x_halo = halo(col_s, col_r, row_s, row_r, diag_r, 0)
    for copy in x_halo:
        copy.start()

    in_g.wait()

    def widen_g(c, carry):
        gflat[pl.ds(pl.multiple_of(c * TH, 8), TH), :] = gin[c].astype(F32)
        return carry

    lax.fori_loop(0, CO, widen_g, 0, unroll=8)

    inner = pl.ds(pl.multiple_of(jnp.where(column == 0, 2 * C, 0), 16), C)

    def patch(dst, cr, rr, dr):
        sides = cr[...].astype(F32)

        def step(h, carry):
            side = pltpu.roll(sides, lax.rem(edge_mine - h + W, W), 1)
            dst[h + 1, inner, :] = jnp.where(lane == edge_mine, side, dst[h + 1, inner, :].astype(F32)).astype(BF16)
            return carry

        lax.fori_loop(0, TH, step, 0, unroll=4)
        build(dst, halo_row - 1, rr[...].astype(F32))
        side = pltpu.roll(dr[...].astype(F32), lax.rem(edge_mine - edge_other + W, W), 1)
        held = dst[halo_row, inner, :].astype(F32)
        dst[halo_row, inner, :] = jnp.where(lane == edge_mine, side, held).astype(BF16)

    for copy in x_halo:
        copy.wait()
    patch(xs, col_r, row_r, diag_r)

    R = 4

    def stack(src, h):
        parts = [src[pl.ds(h + j, 3)].reshape(9 * C, W) for j in range(R)]
        return jnp.concatenate(parts, axis=1)

    def conv(p, carry):
        h = p * R
        block = dot(wfwd[...], stack(xs, h))
        for j in range(R):
            hid[h + j] = block[:, j * W : (j + 1) * W]
        return carry

    lax.fori_loop(0, TH // R, conv, 0)

    def exchange(src, dst, n):
        pltpu.make_async_copy(src, dst.at[me], rsem.at[n]).start()

        for k in peers:
            pltpu.make_async_remote_copy(
                src, dst.at[me], ssem.at[n], rsem.at[n], device_id=peer(k), device_id_type=MESH
            ).start()

    def arrived(dst, n):
        pltpu.make_async_copy(dst, dst, rsem.at[n]).wait()

    def moments(src, depth, message):
        chunk = min(depth, 64)
        firsts, seconds = [], []
        for c in range(0, depth, chunk):
            base = jnp.sum(src[0, c : c + chunk, :], axis=1, keepdims=True) * (1.0 / W)
            shift = jnp.broadcast_to(base, (chunk, W))

            def step(p, carry):
                total, squares = carry
                for j in range(4):
                    v = src[p * 4 + j, c : c + chunk, :] - shift
                    total = total + v
                    squares = squares + v * v
                return total, squares

            zero = jnp.zeros((chunk, W), F32)
            total, squares = lax.fori_loop(0, TH // 4, step, (zero, zero))
            local = jnp.sum(total, axis=1, keepdims=True)
            firsts.append(base + local * (1.0 / n_local))
            seconds.append(jnp.sum(squares, axis=1, keepdims=True) - local * local * (1.0 / n_local))
        put_rows(message, jnp.concatenate(firsts, axis=0), jnp.concatenate(seconds, axis=0))

    def combined(ref, blocks):
        means = ref[:, 0:blocks, :]
        mean = jnp.sum(means, axis=0) * (1.0 / NG)
        off = means - mean[None]
        total = jnp.sum(ref[:, blocks : 2 * blocks, :], axis=0) + n_local * jnp.sum(off * off, axis=0)
        return mean, lax.rsqrt(total * (1.0 / M) + EPS)

    moments(hid, C, m1s)
    exchange(m1s, m1r, 6)

    def lay_out_g(h, carry):
        for c in range(0, CO, 32):
            egrad[h, c : c + 32, :] = gflat[pl.ds(c * TH + h, 32, stride=TH), :]
        return carry

    lax.fori_loop(0, TH, lay_out_g, 0)
    arrived(m1r, 6)
    mean1, scale1 = combined(m1r, nb1)
    gain1, bias1 = vec[0:1, :], vec[1:2, :]
    co1[0] = columns_of(0.5 * gain1 * scale1, C)
    co1[1] = columns_of(0.5 * (bias1 - mean1 * gain1 * scale1), C)

    def activate(p, carry):
        h = p * R
        rows = []
        for j in range(R):
            half = hid[h + j] * co1[0] + co1[1]
            t = jnp.tanh(half)
            u = 1.0 + t
            y = (half * u).astype(BF16)
            hid[h + j] = half
            slope[h + j] = 0.5 * u * (1.0 + half * (1.0 - t))
            ybuf[h + j] = y
            rows.append(y)
        block = dot(wproj[...], jnp.concatenate(rows, axis=1))
        for j in range(R):
            wide[h + j] = block[:, j * W : (j + 1) * W]
        return carry

    lax.fori_loop(0, TH // R, activate, 0)

    moments(wide, CO, m3s)
    exchange(m3s, m3r, 7)

    lt_c = dw.shape[1] // LANES
    lt_p = CO // LANES
    n_conv = C // 16 * lt_c
    n_tiles = n_conv + C // 16 * lt_p

    def scatter(src, dst, low, high, n):
        def send(to):
            owner = to[0] * n_bn + to[1]

            @pl.when(jnp.logical_and(owner >= low, owner < high))
            def _():
                pltpu.make_async_remote_copy(
                    src.at[owner], dst.at[me], ssem.at[n], rsem.at[n], device_id=to, device_id_type=MESH
                ).start()

        @pl.when(jnp.logical_and(me >= low, me < high))
        def _():
            pltpu.make_async_copy(src.at[me], dst.at[me], rsem.at[n]).start()

        for k in peers:
            send(peer(k))

    dh[...] = jnp.zeros_like(dh)

    def weigh(p, carry):
        h = p * R
        ones = jnp.ones((16, W), BF16)
        rows = [jnp.concatenate([hid[h + j].astype(BF16), ones], axis=0) for j in range(R)]
        dh[:, 0 : 9 * C] += dot_nt(jnp.concatenate(rows, axis=1), stack(xs, h))
        return carry

    lax.fori_loop(0, TH // R, weigh, 0)
    for r in range(C // 16):
        for t in range(lt_c):
            cols = slice(t * LANES, (t + 1) * LANES)
            htiles[r * lt_c + t, 0:16, :] = dh[r * 16 : (r + 1) * 16, cols]
            htiles[r * lt_c + t, 16:24, :] = dh[C : C + 8, cols]
    scatter(htiles, rhtiles, 0, n_conv, 14)

    arrived(m3r, 7)
    mean3, scale3 = combined(m3r, nb3)
    gain3, bias3 = vec[2 : 2 + nb3, :], vec[2 + nb3 : 2 + 2 * nb3, :]
    co3[0] = columns_of(0.5 * gain3 * scale3, CO)
    co3[1] = columns_of(0.5 * (bias3 - mean3 * gain3 * scale3), CO)

    step_c = 32
    firsts, seconds = [], []
    for c in range(0, CO, step_c):
        alpha, beta = co3[0, c : c + step_c, :], co3[1, c : c + step_c, :]

        def slopes(p, carry):
            total, cross = carry
            for j in range(4):
                h = p * 4 + j
                half = wide[h, c : c + step_c, :] * alpha + beta
                t = jnp.tanh(half)
                g = egrad[h, c : c + step_c, :]
                e = g * ((1.0 + t) * (1.0 + half * (1.0 - t)))
                wide[h, c : c + step_c, :] = half
                egrad[h, c : c + step_c, :] = e
                total = total + e
                cross = cross + e * half
            return total, cross

        zero = jnp.zeros((step_c, W), F32)
        total, cross = lax.fori_loop(0, TH // 4, slopes, (zero, zero))
        firsts.append(jnp.sum(total, axis=1, keepdims=True))
        seconds.append(jnp.sum(cross, axis=1, keepdims=True))
    put_rows(q3s, jnp.concatenate(firsts, axis=0), jnp.concatenate(seconds, axis=0))
    exchange(q3s, q3r, 8)
    arrived(q3r, 8)
    e_sum = jnp.sum(q3r[:, 0:nb3, :], axis=0)
    eh_sum = jnp.sum(q3r[:, nb3 : 2 * nb3, :], axis=0)
    s3 = 0.5 * e_sum
    q3 = (eh_sum - bias3 * s3) / gain3
    vs[...] = jnp.zeros_like(vs)
    vs[0:nb3, :] = s3
    vs[nb3 : 2 * nb3, :] = q3
    co3[0] = columns_of(0.5 * gain3 * scale3, CO)
    co3[1] = columns_of((-2.0 / M) * scale3 * q3, CO)
    co3[2] = columns_of((1.0 / M) * scale3 * (q3 * bias3 - gain3 * s3), CO)

    pg[...] = jnp.zeros_like(pg)
    dw[...] = jnp.zeros_like(dw)

    def unproject(p, carry):
        total, cross = carry
        h = p * R
        rows = []
        for j in range(R):
            pieces = []
            for c in range(0, CO, 64):
                part = slice(c, c + 64)
                grad = egrad[h + j, part, :] * co3[0, part, :] + wide[h + j, part, :] * co3[1, part, :]
                pieces.append((grad + co3[2, part, :]).astype(BF16))
            rows.append(jnp.concatenate(pieces, axis=0))
        grads = jnp.concatenate(rows, axis=1)
        hidden = jnp.concatenate([ybuf[h + j] for j in range(R)], axis=1)
        pg[...] += dot_nt(hidden, grads)
        block = dot(pw[...], grads)
        rows = []
        for j in range(R):
            e = block[:, j * W : (j + 1) * W] * slope[h + j]
            slope[h + j] = e
            rows.append(e.astype(BF16))
            total = total + e
            cross = cross + e * hid[h + j]
        dw[:, 0 : 9 * C] += dot_nt(jnp.concatenate(rows, axis=1), stack(xs, h))
        return total, cross

    zero = jnp.zeros((C, W), F32)
    total, cross = lax.fori_loop(0, TH // R, unproject, (zero, zero))
    for r in range(C // 16):
        rows = slice(r * 16, (r + 1) * 16)
        for t in range(lt_c):
            tiles[r * lt_c + t] = dw[rows, t * LANES : (t + 1) * LANES]
        for t in range(lt_p):
            tiles[n_conv + r * lt_p + t] = pg[rows, t * LANES : (t + 1) * LANES]
    put_rows(q1s, jnp.sum(total, axis=1, keepdims=True), jnp.sum(cross, axis=1, keepdims=True))
    exchange(q1s, q1r, 9)
    scatter(tiles, rtiles, 0, n_tiles, 10)

    arrived(q1r, 9)
    s1 = jnp.sum(q1r[:, 0:nb1, :], axis=0)
    eh1 = jnp.sum(q1r[:, nb1 : 2 * nb1, :], axis=0)
    safe = jnp.where(lax.broadcasted_iota(jnp.int32, (1, LANES), 1) < C, gain1, 1.0)
    q1 = (2.0 * eh1 - bias1 * s1) / safe
    vs[2 * nb3 : 2 * nb3 + 1, :] = s1
    vs[2 * nb3 + 1 : 2 * nb3 + 2, :] = q1
    co1[0] = columns_of(gain1 * scale1, C)
    co1[1] = columns_of((-2.0 / M) * scale1 * q1, C)
    co1[2] = columns_of((1.0 / M) * scale1 * (q1 * bias1 - gain1 * s1), C)

    def spread(src, dst, n):
        pltpu.make_async_copy(src, dst.at[dp], rsem.at[n]).start()

        for k in others:
            pltpu.make_async_remote_copy(
                src, dst.at[dp], ssem.at[n], rsem.at[n], device_id=across(k), device_id_type=MESH
            ).start()

    spread(vs, vr, 11)

    def unnorm(h, packed):
        row = slope[h] * co1[0] + hid[h] * co1[1] + co1[2]
        slope[h] = row
        build(das, h, row)
        turned = pltpu.roll(row, lax.rem(h - edge_mine + W, W), 1)
        return jnp.where(lane == h, turned, packed)

    dcol_s[...] = lax.fori_loop(0, TH, unnorm, jnp.zeros((C, W), F32), unroll=4).astype(BF16)
    drow_s[...] = slope[row_mine].astype(BF16)
    d_halo = halo(dcol_s, dcol_r, drow_s, drow_r, ddiag_r, 3)
    for copy in d_halo:
        copy.start()

    das[empty_row] = jnp.zeros((3 * C, W), BF16)

    @pl.when(me < n_conv)
    def _():
        arrived(rhtiles, 14)
        arrived(rtiles, 10)
        rows = pl.ds(pl.multiple_of((me // lt_c) * 16, 16), 16)
        whole = jnp.sum(rtiles[...], axis=0) * co1[0, rows, :]
        whole = whole + jnp.sum(rhtiles[:, 0:16, :], axis=0) * co1[1, rows, :]
        whole = whole + jnp.sum(rhtiles[:, 16:17, :], axis=0) * co1[2, rows, :]
        dts[...] = whole.astype(BF16)

    @pl.when(jnp.logical_and(me >= n_conv, me < n_tiles))
    def _():
        arrived(rtiles, 10)
        dts[...] = jnp.sum(rtiles[...], axis=0).astype(BF16)

    @pl.when(me < n_tiles)
    def _():
        spread(dts, dtr, 12)

    for copy in d_halo:
        copy.wait()
    patch(das, dcol_r, drow_r, ddiag_r)

    def unconv(p, carry):
        h = p * R
        block = dot(wbwd[...], stack(das, h))
        for j in range(R):
            flat[pl.ds(h + j, C, stride=TH), :] = block[:, j * W : (j + 1) * W]
        return carry

    lax.fori_loop(0, TH // R, unconv, 0)

    def narrow(c, carry):
        out[c] = flat[pl.ds(pl.multiple_of(c * TH, 8), TH), :].astype(BF16)
        return carry

    lax.fori_loop(0, C, narrow, 0, unroll=4)
    put = pltpu.make_async_copy(out, o_img.at[0, 0], lsem.at[2])
    put.start()

    @pl.when(me < n_tiles)
    def _():
        arrived(dtr, 12)
        ags[...] = (jnp.sum(dtr[...].astype(F32), axis=0) * per_image).astype(BF16)
        exchange(ags, agr, 13)

    arrived(vr, 11)
    o_sums[...] = jnp.sum(vr[...], axis=0) * per_image

    gathered = agr.at[pl.ds(0, n_tiles)]
    pltpu.make_async_copy(gathered, gathered, rsem.at[13]).wait()
    o_agr[...] = agr[0:n_tiles]

    for dst, n in ((m1r, 6), (m3r, 7), (q3r, 8), (q1r, 9)):
        sent = dst.at[pl.ds(0, NG - 1)]
        pltpu.make_async_copy(sent, sent, ssem.at[n]).wait()
    sent = vr.at[pl.ds(0, n_dp - 1)]
    pltpu.make_async_copy(sent, sent, ssem.at[11]).wait()

    @pl.when(me < n_tiles)
    def _():
        sent = rtiles.at[pl.ds(0, n_tiles - 1)]
        pltpu.make_async_copy(sent, sent, ssem.at[10]).wait()
        sent = dtr.at[pl.ds(0, n_dp - 1)]
        pltpu.make_async_copy(sent, sent, ssem.at[12]).wait()
        sent = agr.at[pl.ds(0, NG - 1)]
        pltpu.make_async_copy(sent, sent, ssem.at[13]).wait()

    @pl.when(me >= n_tiles)
    def _():
        sent = rtiles.at[pl.ds(0, n_tiles)]
        pltpu.make_async_copy(sent, sent, ssem.at[10]).wait()

    @pl.when(me < n_conv)
    def _():
        sent = rhtiles.at[pl.ds(0, n_conv - 1)]
        pltpu.make_async_copy(sent, sent, ssem.at[14]).wait()

    @pl.when(me >= n_conv)
    def _():
        sent = rhtiles.at[pl.ds(0, n_conv)]
        pltpu.make_async_copy(sent, sent, ssem.at[14]).wait()

    put.wait()


def finish(img, agr, sums, o_img, o_cw, o_pw, o_g1, o_b1, o_g3, o_b3, sem):
    copy = pltpu.make_async_copy(img, o_img, sem)
    copy.start()
    C = o_pw.shape[0]
    nb3 = o_g3.shape[0]
    lt_p = o_pw.shape[1] // LANES
    lt_c = -(-9 * C // LANES)
    n_conv = C // 16 * lt_c
    o_b3[...] = sums[0:nb3]
    o_g3[...] = sums[nb3 : 2 * nb3]
    o_b1[...] = sums[2 * nb3 : 2 * nb3 + 1, 0:C]
    o_g1[...] = sums[2 * nb3 + 1 : 2 * nb3 + 2, 0:C]
    for r in range(C // 16):
        rows = slice(r * 16, (r + 1) * 16)
        for t in range(lt_p):
            o_pw[rows, t * LANES : (t + 1) * LANES] = agr[n_conv + r * lt_p + t].astype(F32)
        line = [agr[r * lt_c + t].astype(F32) for t in range(lt_c)]
        line = jnp.concatenate(line, axis=1)
        for n in range(9):
            o_cw[n // 3, n % 3, rows, :] = line[:, n * C : (n + 1) * C]
    copy.wait()


def solution(mesh):
    n_sp, n_bn, n_dp = mesh.shape["sp"], mesh.shape["bn"], mesh.shape["dp"]
    NG = n_sp * n_bn

    def step(images, out_grad, conv_weight, proj_weight, gain_one, shift_one, gain_three, shift_three):
        C, TH, W = images.shape[2:]
        CO = out_grad.shape[2]
        nb1, nb3 = 1, CO // LANES
        wide_c = -(-9 * C // LANES) * LANES
        n_conv = C // 16 * (wide_c // LANES)
        n_tiles = n_conv + C // 16 * (CO // LANES)
        vm = pltpu.VMEM
        scratch = [
            vm((C, TH, W), BF16), vm((CO, TH, W), BF16), vm((C * TH, W), F32), vm((CO * TH, W), F32),
            vm((TH + 2, 3 * C, W), BF16), vm((TH, C, W), F32), vm((TH, C, W), F32), vm((TH, C, W), BF16),
            vm((TH, CO, W), F32), vm((TH, CO, W), F32), vm((TH + 2, 3 * C, W), BF16), vm((C, TH, W), BF16),
            vm((C, 9 * C), BF16), vm((C, 9 * C), BF16), vm((CO, C), BF16),
            *[vm((C, W), BF16) for _ in range(10)][:5], *[vm((C, W), BF16) for _ in range(5)],
            vm((2 * nb1, LANES), F32), vm((NG, 2 * nb1, LANES), F32),
            vm((2 * nb3, LANES), F32), vm((NG, 2 * nb3, LANES), F32),
            vm((2 * nb3, LANES), F32), vm((NG, 2 * nb3, LANES), F32),
            vm((2 * nb1, LANES), F32), vm((NG, 2 * nb1, LANES), F32),
            vm((C, wide_c), F32), vm((C, CO), F32), vm((n_tiles, 16, LANES), F32), vm((NG, 16, LANES), F32),
            vm((16, LANES), BF16), vm((n_dp, 16, LANES), BF16), vm((8, LANES), F32), vm((n_dp, 8, LANES), F32),
            vm((16, LANES), BF16), vm((NG, 16, LANES), BF16), vm((8, LANES), F32),
            vm((3, CO, W), F32), vm((3, C, W), F32),
            vm((C + 16, wide_c), F32), vm((n_conv, 24, LANES), F32), vm((NG, 24, LANES), F32),
            pltpu.SemaphoreType.DMA((15,)), pltpu.SemaphoreType.DMA((15,)), pltpu.SemaphoreType.DMA((3,)),
        ]
        vspec = pl.BlockSpec(memory_space=pltpu.VMEM)
        aspec = pl.BlockSpec(memory_space=pl.ANY)
        hspec = pl.BlockSpec(memory_space=pltpu.HBM)
        shape = jax.ShapeDtypeStruct
        img, tiles, sums = pl.pallas_call(
            functools.partial(kernel, n_sp, n_bn, n_dp, 1.0 / float(n_sp * TH * W)),
            out_shape=(shape(images.shape, BF16), shape((n_tiles, 16, LANES), BF16), shape((8, LANES), F32)),
            in_specs=[hspec, hspec] + [vspec] * 6,
            out_specs=(aspec, vspec, vspec),
            scratch_shapes=scratch,
            compiler_params=pltpu.CompilerParams(
                collective_id=0, has_side_effects=True, vmem_limit_bytes=55200000
            ),
        )(
            images, out_grad, conv_weight, proj_weight, gain_one.reshape(1, C), shift_one.reshape(1, C),
            gain_three.reshape(nb3, LANES), shift_three.reshape(nb3, LANES),
        )
        got = pl.pallas_call(
            finish,
            out_shape=(
                shape(images.shape, BF16), shape((3, 3, C, C), F32), shape((C, CO), F32), shape((1, C), F32),
                shape((1, C), F32), shape((nb3, LANES), F32), shape((nb3, LANES), F32),
            ),
            in_specs=[aspec, vspec, vspec],
            out_specs=(aspec,) + (vspec,) * 6,
            scratch_shapes=[pltpu.SemaphoreType.DMA],
            compiler_params=pltpu.CompilerParams(vmem_limit_bytes=4 * 1024 * 1024),
        )(img, tiles, sums)
        return (
            got[0], got[1], got[2], got[3].reshape(C), got[4].reshape(C), got[5].reshape(CO), got[6].reshape(CO),
        )

    split = P(("bn", "dp"), "sp", None, None, None)
    return jax.shard_map(
        step,
        mesh=mesh,
        in_specs=(split, split) + (P(),) * 6,
        out_specs=(split,) + (P(),) * 6,
        check_vma=False,
    )
```

```python
import functools

import jax
import jax.numpy as jnp
from jax import lax
from jax.experimental import pallas as pl
from jax.experimental.pallas import tpu as pltpu
from jax.sharding import PartitionSpec as P

MESH = pl.DeviceIdType.MESH
F32 = jnp.float32
BF16 = jnp.bfloat16
EPS = 1e-05
LANES = 128


def dot(a, b):
    return lax.dot_general(a, b, (((1,), (0,)), ((), ())), preferred_element_type=F32)


def dot_nt(a, b):
    return lax.dot_general(a, b, (((1,), (1,)), ((), ())), preferred_element_type=F32)


def to_column(row):
    return jnp.transpose(jnp.broadcast_to(row, (LANES, LANES)))


def columns_of(rows, depth):
    parts = [to_column(rows[k : k + 1]) for k in range(rows.shape[0])]
    return jnp.concatenate(parts, axis=0)[:depth] if len(parts) > 1 else parts[0][:depth]


def put_rows(ref, first, second):
    depth = first.shape[0]
    blocks = ref.shape[0] // 2
    lane = lax.broadcasted_iota(jnp.int32, (depth, LANES), 1)
    table = jnp.where(lane == 0, first, jnp.where(lane == 1, second, 0.0))
    if depth < LANES:
        table = jnp.concatenate([table, jnp.zeros((LANES - depth, LANES), F32)], axis=0)
    for k in range(blocks):
        turned = jnp.transpose(table[k * LANES : (k + 1) * LANES])
        ref[k : k + 1, :] = turned[0:1]
        ref[blocks + k : blocks + k + 1, :] = turned[1:2]


def kernel(
    n_sp, n_bn, n_dp, per_image,
    img, cot, cw_in, pw_in, g1_in, b1_in, g3_in, b3_in,
    o_img, o_agr, o_sums,
    xin, gin, flat, gflat, xs, hid, slope, ybuf, wide, egrad, das, out,
    wfwd, wbwd, wproj, col_s, col_r, row_r, diag_r, row_s, dcol_s, dcol_r, drow_s, drow_r, ddiag_r,
    m1s, m1r, m3s, m3r, q3s, q3r, q1s, q1r, dw, pg, tiles, rtiles, dts, dtr, vs, vr, ags, agr, vec,
    co3, co1, dh, htiles, rhtiles, gram, ebuf,
    cw, pw, g1, b1, g3, b3, rsem, ssem, lsem,
):
    C, TH, W = xin.shape
    CO = gin.shape[0]
    NG = n_sp * n_bn
    nb1, nb3 = m1s.shape[0] // 2, m3s.shape[0] // 2
    n_local = float(TH * W)
    M = n_local * NG
    sp, bn, dp = lax.axis_index("sp"), lax.axis_index("bn"), lax.axis_index("dp")
    me = sp * n_bn + bn
    column = lax.rem(sp, 2)
    rowhalf = sp // 2

    def wrapped(at, step, size):
        moved = at + step
        return jnp.where(moved >= size, moved - size, moved)

    xs_of = [wrapped(sp, k, n_sp) for k in range(n_sp)]
    zs_of = [wrapped(bn, k, n_bn) for k in range(n_bn)]
    ds_of = [wrapped(dp, k, n_dp) for k in range(n_dp)]

    def ring(step, size):
        return min(step, size - step)

    peers = sorted(range(1, NG), key=lambda k: -ring(k // n_bn, n_sp) - ring(k % n_bn, n_bn))
    others = sorted(range(1, n_dp), key=lambda k: -ring(k // 2, n_dp // 2))

    def peer(k):
        return (xs_of[k // n_bn], zs_of[k % n_bn], dp)

    def across(k):
        return (sp, bn, ds_of[k])

    in_x = pltpu.make_async_copy(img.at[0, 0], xin, lsem.at[0])
    in_g = pltpu.make_async_copy(cot.at[0, 0], gin, lsem.at[1])
    pairs = ((cw_in, cw), (pw_in, pw), (g1_in, g1), (b1_in, b1), (g3_in, g3), (b3_in, b3))
    small = [pltpu.make_async_copy(src, dst, lsem.at[3 + i]) for i, (src, dst) in enumerate(pairs)]
    in_x.start()
    for copy in small:
        copy.start()
    in_g.start()

    barrier = pltpu.get_barrier_semaphore()

    for k in peers:
        pl.semaphore_signal(barrier, inc=1, device_id=peer(k), device_id_type=MESH)
    for k in others:
        pl.semaphore_signal(barrier, inc=1, device_id=across(k), device_id_type=MESH)

    for copy in small:
        copy.wait()
    taps = [cw[n // 3, n % 3].astype(F32) for n in range(9)]
    wfwd[...] = jnp.concatenate(taps, axis=1).astype(BF16)
    flipped = jnp.concatenate([taps[8 - n] for n in range(9)], axis=0)
    wbwd[...] = jnp.transpose(flipped).astype(BF16)
    wproj[...] = jnp.transpose(pw[...].astype(F32)).astype(BF16)
    vec[...] = jnp.zeros_like(vec)
    vec[0:1, 0:C] = g1[...]
    vec[1:2, 0:C] = b1[...]
    vec[2 : 2 + nb3, :] = g3[...]
    vec[2 + nb3 : 2 + 2 * nb3, :] = b3[...]

    in_x.wait()

    def widen(c, carry):
        flat[pl.ds(pl.multiple_of(c * TH, 8), TH), :] = xin[c].astype(F32)
        return carry

    lax.fori_loop(0, C, widen, 0, unroll=4)

    lane = lax.broadcasted_iota(jnp.int32, (C, W), 1)
    edge_mine = jnp.where(column == 0, W - 1, 0)
    edge_other = (W - 1) - edge_mine
    row_mine = jnp.where(rowhalf == 0, TH - 1, 0)
    halo_row = jnp.where(rowhalf == 0, TH + 1, 0)
    empty_row = (TH + 1) - halo_row

    def pick(h):
        return flat[pl.ds(h, C, stride=TH), :]

    def gather_column(row_of):
        def step(h, packed):
            turned = pltpu.roll(row_of(h), lax.rem(h - edge_mine + W, W), 1)
            return jnp.where(lane == h, turned, packed)

        return lax.fori_loop(0, TH, step, jnp.zeros((C, W), F32), unroll=4)

    col_s[...] = gather_column(pick).astype(BF16)
    row_s[...] = pick(row_mine).astype(BF16)

    def build(dst, h, row):
        left = jnp.where(lane == 0, 0.0, pltpu.roll(row, 1, 1))
        right = jnp.where(lane == W - 1, 0.0, pltpu.roll(row, W - 1, 1))
        dst[h + 1, 0:C, :] = left.astype(BF16)
        dst[h + 1, C : 2 * C, :] = row.astype(BF16)
        dst[h + 1, 2 * C : 3 * C, :] = right.astype(BF16)

    def lay_out(h, carry):
        build(xs, h, pick(h))
        return carry

    lax.fori_loop(0, TH, lay_out, 0, unroll=4)
    xs[empty_row] = jnp.zeros((3 * C, W), BF16)

    pl.semaphore_wait(barrier, NG - 1 + n_dp - 1)

    beside = (sp + 1 - 2 * column, bn, dp)
    below = (lax.rem(sp + 2, 4), bn, dp)
    corner = (3 - sp, bn, dp)

    def halo(cs, cr, rs, rr, dr, base):
        return [
            pltpu.make_async_remote_copy(cs, cr, ssem.at[base], rsem.at[base], device_id=beside, device_id_type=MESH),
            pltpu.make_async_remote_copy(
                rs, rr, ssem.at[base + 1], rsem.at[base + 1], device_id=below, device_id_type=MESH
            ),
            pltpu.make_async_remote_copy(
                rs, dr, ssem.at[base + 2], rsem.at[base + 2], device_id=corner, device_id_type=MESH
            ),
        ]

    x_halo = halo(col_s, col_r, row_s, row_r, diag_r, 0)
    for copy in x_halo:
        copy.start()

    in_g.wait()

    def widen_g(c, carry):
        gflat[pl.ds(pl.multiple_of(c * TH, 8), TH), :] = gin[c].astype(F32)
        return carry

    lax.fori_loop(0, CO, widen_g, 0, unroll=8)

    inner = pl.ds(pl.multiple_of(jnp.where(column == 0, 2 * C, 0), 16), C)

    def patch(dst, cr, rr, dr):
        sides = cr[...].astype(F32)

        def step(h, carry):
            side = pltpu.roll(sides, lax.rem(edge_mine - h + W, W), 1)
            dst[h + 1, inner, :] = jnp.where(lane == edge_mine, side, dst[h + 1, inner, :].astype(F32)).astype(BF16)
            return carry

        lax.fori_loop(0, TH, step, 0, unroll=4)
        build(dst, halo_row - 1, rr[...].astype(F32))
        side = pltpu.roll(dr[...].astype(F32), lax.rem(edge_mine - edge_other + W, W), 1)
        held = dst[halo_row, inner, :].astype(F32)
        dst[halo_row, inner, :] = jnp.where(lane == edge_mine, side, held).astype(BF16)

    for copy in x_halo:
        copy.wait()
    patch(xs, col_r, row_r, diag_r)

    R = 4

    def stack(src, h):
        parts = [src[pl.ds(h + j, 3)].reshape(9 * C, W) for j in range(R)]
        return jnp.concatenate(parts, axis=1)

    def conv(p, carry):
        h = p * R
        block = dot(wfwd[...], stack(xs, h))
        for j in range(R):
            hid[h + j] = block[:, j * W : (j + 1) * W]
        return carry

    lax.fori_loop(0, TH // R, conv, 0)

    def exchange(src, dst, n):
        pltpu.make_async_copy(src, dst.at[me], rsem.at[n]).start()

        for k in peers:
            pltpu.make_async_remote_copy(
                src, dst.at[me], ssem.at[n], rsem.at[n], device_id=peer(k), device_id_type=MESH
            ).start()

    def arrived(dst, n):
        pltpu.make_async_copy(dst, dst, rsem.at[n]).wait()

    def moments(src, depth, message):
        chunk = min(depth, 64)
        firsts, seconds = [], []
        for c in range(0, depth, chunk):
            base = jnp.sum(src[0, c : c + chunk, :], axis=1, keepdims=True) * (1.0 / W)
            shift = jnp.broadcast_to(base, (chunk, W))

            def step(p, carry):
                total, squares = carry
                for j in range(4):
                    v = src[p * 4 + j, c : c + chunk, :] - shift
                    total = total + v
                    squares = squares + v * v
                return total, squares

            zero = jnp.zeros((chunk, W), F32)
            total, squares = lax.fori_loop(0, TH // 4, step, (zero, zero))
            local = jnp.sum(total, axis=1, keepdims=True)
            firsts.append(base + local * (1.0 / n_local))
            seconds.append(jnp.sum(squares, axis=1, keepdims=True) - local * local * (1.0 / n_local))
        put_rows(message, jnp.concatenate(firsts, axis=0), jnp.concatenate(seconds, axis=0))

    def combined(ref, blocks):
        means = ref[:, 0:blocks, :]
        mean = jnp.sum(means, axis=0) * (1.0 / NG)
        off = means - mean[None]
        total = jnp.sum(ref[:, blocks : 2 * blocks, :], axis=0) + n_local * jnp.sum(off * off, axis=0)
        return mean, lax.rsqrt(total * (1.0 / M) + EPS)

    moments(hid, C, m1s)
    exchange(m1s, m1r, 6)

    def lay_out_g(h, carry):
        for c in range(0, CO, 32):
            egrad[h, c : c + 32, :] = gflat[pl.ds(c * TH + h, 32, stride=TH), :]
        return carry

    lax.fori_loop(0, TH, lay_out_g, 0)
    arrived(m1r, 6)
    mean1, scale1 = combined(m1r, nb1)
    gain1, bias1 = vec[0:1, :], vec[1:2, :]
    co1[0] = columns_of(0.5 * gain1 * scale1, C)
    co1[1] = columns_of(0.5 * (bias1 - mean1 * gain1 * scale1), C)
    middle = jnp.floor(bias1 * (8.0 + 8.0 * jnp.tanh(0.5 * bias1)) + 0.5) * (1.0 / 16.0)
    co1[2] = columns_of(middle, C)
    gram[...] = jnp.zeros_like(gram)

    def activate(p, carry):
        h = p * R
        rows = []
        for j in range(R):
            half = hid[h + j] * co1[0] + co1[1]
            t = jnp.tanh(half)
            u = 1.0 + t
            y = (half * u).astype(BF16)
            hid[h + j] = half
            slope[h + j] = 0.5 * u * (1.0 + half * (1.0 - t))
            ybuf[h + j] = y
            rows.append((y.astype(F32) - co1[2]).astype(BF16))
        off = jnp.concatenate(rows, axis=1)
        gram[...] += dot_nt(jnp.concatenate([off, jnp.ones((16, R * W), BF16)], axis=0), off)
        return carry

    lax.fori_loop(0, TH // R, activate, 0)
    gram[C : C + 8, :] = gram[C : C + 8, :] * (1.0 / n_local)
    gram[C + 8 : C + 16, :] = jnp.broadcast_to(middle[:, 0:C], (8, C))
    table = gram[...]
    high = table.astype(BF16)
    rest = table - high.astype(F32)
    mid = rest.astype(BF16)
    low = (rest - mid.astype(F32)).astype(BF16)
    turned = dot(jnp.concatenate([high, mid, low], axis=0), pw[...])
    turned = turned[0 : C + 16] + turned[C + 16 : 2 * C + 32] + turned[2 * C + 32 :]
    local = turned[C : C + 1]
    spread_of = jnp.sum(turned[0:C] * pw[...].astype(F32), axis=0, keepdims=True) - n_local * local * local
    local = local + turned[C + 8 : C + 9]
    for k in range(nb3):
        m3s[k : k + 1, :] = local[:, k * LANES : (k + 1) * LANES]
        m3s[nb3 + k : nb3 + k + 1, :] = spread_of[:, k * LANES : (k + 1) * LANES]
    exchange(m3s, m3r, 7)

    def project(p, carry):
        h = p * R
        block = dot(wproj[...], jnp.concatenate([ybuf[h + j] for j in range(R)], axis=1))
        for j in range(R):
            wide[h + j] = block[:, j * W : (j + 1) * W]
        return carry

    lax.fori_loop(0, TH // R, project, 0)

    lt_c = dw.shape[1] // LANES
    lt_p = CO // LANES
    n_conv = C // 16 * lt_c
    n_tiles = n_conv + C // 16 * lt_p

    def scatter(src, dst, low, high, n):
        def send(to):
            owner = to[0] * n_bn + to[1]

            @pl.when(jnp.logical_and(owner >= low, owner < high))
            def _():
                pltpu.make_async_remote_copy(
                    src.at[owner], dst.at[me], ssem.at[n], rsem.at[n], device_id=to, device_id_type=MESH
                ).start()

        @pl.when(jnp.logical_and(me >= low, me < high))
        def _():
            pltpu.make_async_copy(src.at[me], dst.at[me], rsem.at[n]).start()

        for k in peers:
            send(peer(k))

    dh[...] = jnp.zeros_like(dh)

    def weigh(p, carry):
        h = p * R
        ones = jnp.ones((16, W), BF16)
        rows = [jnp.concatenate([hid[h + j].astype(BF16), ones], axis=0) for j in range(R)]
        dh[:, 0 : 9 * C] += dot_nt(jnp.concatenate(rows, axis=1), stack(xs, h))
        return carry

    lax.fori_loop(0, TH // R, weigh, 0)
    for r in range(C // 16):
        for t in range(lt_c):
            cols = slice(t * LANES, (t + 1) * LANES)
            htiles[r * lt_c + t, 0:16, :] = dh[r * 16 : (r + 1) * 16, cols]
            htiles[r * lt_c + t, 16:24, :] = dh[C : C + 8, cols]
    scatter(htiles, rhtiles, 0, n_conv, 14)

    arrived(m3r, 7)
    mean3, scale3 = combined(m3r, nb3)
    gain3, bias3 = vec[2 : 2 + nb3, :], vec[2 + nb3 : 2 + 2 * nb3, :]
    co3[0] = columns_of(0.5 * gain3 * scale3, CO)
    co3[1] = columns_of(0.5 * (bias3 - mean3 * gain3 * scale3), CO)

    step_c = 32
    firsts, seconds = [], []
    for c in range(0, CO, step_c):
        alpha, beta = co3[0, c : c + step_c, :], co3[1, c : c + step_c, :]

        def slopes(p, carry):
            total, cross = carry
            for j in range(8):
                h = p * 8 + j
                half = wide[h, c : c + step_c, :] * alpha + beta
                t = jnp.tanh(half)
                g = egrad[h, c : c + step_c, :]
                e = g * ((1.0 + t) * (1.0 + half * (1.0 - t)))
                wide[h, c : c + step_c, :] = half
                egrad[h, c : c + step_c, :] = e
                total = total + e
                cross = cross + e * half
            return total, cross

        zero = jnp.zeros((step_c, W), F32)
        total, cross = lax.fori_loop(0, TH // 8, slopes, (zero, zero))
        firsts.append(jnp.sum(total, axis=1, keepdims=True))
        seconds.append(jnp.sum(cross, axis=1, keepdims=True))
    put_rows(q3s, jnp.concatenate(firsts, axis=0), jnp.concatenate(seconds, axis=0))
    exchange(q3s, q3r, 8)
    arrived(q3r, 8)
    e_sum = jnp.sum(q3r[:, 0:nb3, :], axis=0)
    eh_sum = jnp.sum(q3r[:, nb3 : 2 * nb3, :], axis=0)
    s3 = 0.5 * e_sum
    q3 = (eh_sum - bias3 * s3) / gain3
    vs[...] = jnp.zeros_like(vs)
    vs[0:nb3, :] = s3
    vs[nb3 : 2 * nb3, :] = q3
    co3[1] = columns_of((-2.0 / M) * scale3 * q3, CO)
    co3[2] = columns_of((1.0 / M) * scale3 * (q3 * bias3 - gain3 * s3), CO)

    pg[...] = jnp.zeros_like(pg)
    dw[...] = jnp.zeros_like(dw)
    ebuf[...] = jnp.zeros_like(ebuf)

    def max_of(p):
        return jnp.where(p < 0, 0, p)

    def unproject(p, carry):
        total, cross = carry
        h = p * R
        pieces = []
        for c in range(0, CO, 32):
            part = slice(c, c + 32)
            alpha, beta, gamma = co3[0, part, :], co3[1, part, :], co3[2, part, :]
            rows = [
                (egrad[h + j, part, :] * alpha + wide[h + j, part, :] * beta + gamma).astype(BF16) for j in range(R)
            ]
            pieces.append(jnp.concatenate(rows, axis=1))
        grads = jnp.concatenate(pieces, axis=0)
        hidden = jnp.concatenate([ybuf[h + j] for j in range(R)], axis=1)
        pg[...] += dot_nt(hidden, grads)
        block = dot(pw[...], grads)
        held = max_of(p - 1) * R
        dw[:, 0 : 9 * C] += dot_nt(ebuf[...], stack(xs, held))
        rows = []
        for j in range(R):
            e = block[:, j * W : (j + 1) * W] * slope[h + j]
            slope[h + j] = e
            rows.append(e.astype(BF16))
            total = total + e
            cross = cross + e * hid[h + j]
        ebuf[...] = jnp.concatenate(rows, axis=1)
        return total, cross

    zero = jnp.zeros((C, W), F32)
    total, cross = lax.fori_loop(0, TH // R, unproject, (zero, zero))
    dw[:, 0 : 9 * C] += dot_nt(ebuf[...], stack(xs, TH - R))

    for r in range(C // 16):
        rows = slice(r * 16, (r + 1) * 16)
        for t in range(lt_c):
            tiles[r * lt_c + t] = dw[rows, t * LANES : (t + 1) * LANES]
        for t in range(lt_p):
            tiles[n_conv + r * lt_p + t] = pg[rows, t * LANES : (t + 1) * LANES]
    scatter(tiles, rtiles, 0, n_tiles, 10)
    put_rows(q1s, jnp.sum(total, axis=1, keepdims=True), jnp.sum(cross, axis=1, keepdims=True))
    exchange(q1s, q1r, 9)

    arrived(q1r, 9)
    s1 = jnp.sum(q1r[:, 0:nb1, :], axis=0)
    eh1 = jnp.sum(q1r[:, nb1 : 2 * nb1, :], axis=0)
    safe = jnp.where(lax.broadcasted_iota(jnp.int32, (1, LANES), 1) < C, gain1, 1.0)
    q1 = (2.0 * eh1 - bias1 * s1) / safe
    vs[2 * nb3 : 2 * nb3 + 1, :] = s1
    vs[2 * nb3 + 1 : 2 * nb3 + 2, :] = q1
    co1[0] = columns_of(gain1 * scale1, C)
    co1[1] = columns_of((-2.0 / M) * scale1 * q1, C)
    co1[2] = columns_of((1.0 / M) * scale1 * (q1 * bias1 - gain1 * s1), C)

    def spread(src, dst, n):
        pltpu.make_async_copy(src, dst.at[dp], rsem.at[n]).start()

        for k in others:
            pltpu.make_async_remote_copy(
                src, dst.at[dp], ssem.at[n], rsem.at[n], device_id=across(k), device_id_type=MESH
            ).start()

    spread(vs, vr, 11)

    def unnorm(h, packed):
        row = slope[h] * co1[0] + hid[h] * co1[1] + co1[2]
        slope[h] = row
        build(das, h, row)
        turned = pltpu.roll(row, lax.rem(h - edge_mine + W, W), 1)
        return jnp.where(lane == h, turned, packed)

    dcol_s[...] = lax.fori_loop(0, TH, unnorm, jnp.zeros((C, W), F32), unroll=4).astype(BF16)
    drow_s[...] = slope[row_mine].astype(BF16)
    d_halo = halo(dcol_s, dcol_r, drow_s, drow_r, ddiag_r, 3)
    for copy in d_halo:
        copy.start()

    das[empty_row] = jnp.zeros((3 * C, W), BF16)

    @pl.when(me < n_conv)
    def _():
        arrived(rhtiles, 14)
        arrived(rtiles, 10)
        rows = pl.ds(pl.multiple_of((me // lt_c) * 16, 16), 16)
        whole = jnp.sum(rtiles[...], axis=0) * co1[0, rows, :]
        whole = whole + jnp.sum(rhtiles[:, 0:16, :], axis=0) * co1[1, rows, :]
        whole = whole + jnp.sum(rhtiles[:, 16:17, :], axis=0) * co1[2, rows, :]
        dts[...] = whole.astype(BF16)

    @pl.when(jnp.logical_and(me >= n_conv, me < n_tiles))
    def _():
        arrived(rtiles, 10)
        dts[...] = jnp.sum(rtiles[...], axis=0).astype(BF16)

    @pl.when(me < n_tiles)
    def _():
        spread(dts, dtr, 12)

    for copy in d_halo:
        copy.wait()
    patch(das, dcol_r, drow_r, ddiag_r)

    def unconv(p, carry):
        h = p * R
        block = dot(wbwd[...], stack(das, h))
        for j in range(R):
            flat[pl.ds(h + j, C, stride=TH), :] = block[:, j * W : (j + 1) * W]
        return carry

    lax.fori_loop(0, TH // R, unconv, 0)

    def narrow(c, carry):
        out[c] = flat[pl.ds(pl.multiple_of(c * TH, 8), TH), :].astype(BF16)
        return carry

    lax.fori_loop(0, C, narrow, 0, unroll=4)
    put = pltpu.make_async_copy(out, o_img.at[0, 0], lsem.at[2])
    put.start()

    @pl.when(me < n_tiles)
    def _():
        arrived(dtr, 12)
        ags[...] = (jnp.sum(dtr[...].astype(F32), axis=0) * per_image).astype(BF16)
        exchange(ags, agr, 13)

    arrived(vr, 11)
    o_sums[...] = jnp.sum(vr[...], axis=0) * per_image

    gathered = agr.at[pl.ds(0, n_tiles)]
    pltpu.make_async_copy(gathered, gathered, rsem.at[13]).wait()
    o_agr[...] = agr[0:n_tiles]

    for dst, n in ((m1r, 6), (m3r, 7), (q3r, 8), (q1r, 9)):
        sent = dst.at[pl.ds(0, NG - 1)]
        pltpu.make_async_copy(sent, sent, ssem.at[n]).wait()
    sent = vr.at[pl.ds(0, n_dp - 1)]
    pltpu.make_async_copy(sent, sent, ssem.at[11]).wait()

    @pl.when(me < n_tiles)
    def _():
        sent = rtiles.at[pl.ds(0, n_tiles - 1)]
        pltpu.make_async_copy(sent, sent, ssem.at[10]).wait()
        sent = dtr.at[pl.ds(0, n_dp - 1)]
        pltpu.make_async_copy(sent, sent, ssem.at[12]).wait()
        sent = agr.at[pl.ds(0, NG - 1)]
        pltpu.make_async_copy(sent, sent, ssem.at[13]).wait()

    @pl.when(me >= n_tiles)
    def _():
        sent = rtiles.at[pl.ds(0, n_tiles)]
        pltpu.make_async_copy(sent, sent, ssem.at[10]).wait()

    @pl.when(me < n_conv)
    def _():
        sent = rhtiles.at[pl.ds(0, n_conv - 1)]
        pltpu.make_async_copy(sent, sent, ssem.at[14]).wait()

    @pl.when(me >= n_conv)
    def _():
        sent = rhtiles.at[pl.ds(0, n_conv)]
        pltpu.make_async_copy(sent, sent, ssem.at[14]).wait()

    put.wait()


def finish(img, agr_in, sums_in, o_img, o_cw, o_pw, o_g1, o_b1, o_g3, o_b3, held, agr, sums, sem):
    small = [pltpu.make_async_copy(agr_in, agr, sem.at[0]), pltpu.make_async_copy(sums_in, sums, sem.at[1])]
    parts = 4
    step = held.shape[0] // parts
    cuts = [pl.ds(k * step, step) for k in range(parts)]
    come = [pltpu.make_async_copy(img.at[0, 0, c], held.at[c], sem.at[2 + k]) for k, c in enumerate(cuts)]
    leave = [pltpu.make_async_copy(held.at[c], o_img.at[0, 0, c], sem.at[2 + parts + k]) for k, c in enumerate(cuts)]
    for copy in small + come:
        copy.start()
    for there, back in zip(come, leave):
        there.wait()
        back.start()
    for copy in small:
        copy.wait()
    C = o_pw.shape[0]
    nb3 = o_g3.shape[0]
    lt_p = o_pw.shape[1] // LANES
    lt_c = -(-9 * C // LANES)
    n_conv = C // 16 * lt_c
    o_b3[...] = sums[0:nb3]
    o_g3[...] = sums[nb3 : 2 * nb3]
    o_b1[...] = sums[2 * nb3 : 2 * nb3 + 1, 0:C]
    o_g1[...] = sums[2 * nb3 + 1 : 2 * nb3 + 2, 0:C]
    for r in range(C // 16):
        rows = slice(r * 16, (r + 1) * 16)
        for t in range(lt_p):
            o_pw[rows, t * LANES : (t + 1) * LANES] = agr[n_conv + r * lt_p + t].astype(F32)
        line = [agr[r * lt_c + t].astype(F32) for t in range(lt_c)]
        line = jnp.concatenate(line, axis=1)
        for n in range(9):
            o_cw[n // 3, n % 3, rows, :] = line[:, n * C : (n + 1) * C]
    for copy in leave:
        copy.wait()


def solution(mesh):
    n_sp, n_bn, n_dp = mesh.shape["sp"], mesh.shape["bn"], mesh.shape["dp"]
    NG = n_sp * n_bn

    def step(images, out_grad, conv_weight, proj_weight, gain_one, shift_one, gain_three, shift_three):
        C, TH, W = images.shape[2:]
        CO = out_grad.shape[2]
        nb1, nb3 = 1, CO // LANES
        wide_c = -(-9 * C // LANES) * LANES
        n_conv = C // 16 * (wide_c // LANES)
        n_tiles = n_conv + C // 16 * (CO // LANES)
        vm = pltpu.VMEM
        scratch = [
            vm((C, TH, W), BF16), vm((CO, TH, W), BF16), vm((C * TH, W), F32), vm((CO * TH, W), F32),
            vm((TH + 2, 3 * C, W), BF16), vm((TH, C, W), F32), vm((TH, C, W), F32), vm((TH, C, W), BF16),
            vm((TH, CO, W), F32), vm((TH, CO, W), F32), vm((TH + 2, 3 * C, W), BF16), vm((C, TH, W), BF16),
            vm((C, 9 * C), BF16), vm((C, 9 * C), BF16), vm((CO, C), BF16),
            *[vm((C, W), BF16) for _ in range(10)][:5], *[vm((C, W), BF16) for _ in range(5)],
            vm((2 * nb1, LANES), F32), vm((NG, 2 * nb1, LANES), F32),
            vm((2 * nb3, LANES), F32), vm((NG, 2 * nb3, LANES), F32),
            vm((2 * nb3, LANES), F32), vm((NG, 2 * nb3, LANES), F32),
            vm((2 * nb1, LANES), F32), vm((NG, 2 * nb1, LANES), F32),
            vm((C, wide_c), F32), vm((C, CO), F32), vm((n_tiles, 16, LANES), F32), vm((NG, 16, LANES), F32),
            vm((16, LANES), BF16), vm((n_dp, 16, LANES), BF16), vm((8, LANES), F32), vm((n_dp, 8, LANES), F32),
            vm((16, LANES), BF16), vm((NG, 16, LANES), BF16), vm((8, LANES), F32),
            vm((3, CO, W), F32), vm((3, C, W), F32),
            vm((C + 16, wide_c), F32), vm((n_conv, 24, LANES), F32), vm((NG, 24, LANES), F32), vm((C + 16, C), F32), vm((C, 4 * W), BF16),
            vm((3, 3, C, C), BF16), vm((C, CO), BF16), vm((1, C), F32), vm((1, C), F32), vm((nb3, LANES), F32),
            vm((nb3, LANES), F32),
            pltpu.SemaphoreType.DMA((15,)), pltpu.SemaphoreType.DMA((15,)), pltpu.SemaphoreType.DMA((9,)),
        ]
        vspec = pl.BlockSpec(memory_space=pltpu.VMEM)
        aspec = pl.BlockSpec(memory_space=pl.ANY)
        shape = jax.ShapeDtypeStruct
        img, tiles, sums = pl.pallas_call(
            functools.partial(kernel, n_sp, n_bn, n_dp, 1.0 / float(n_sp * TH * W)),
            out_shape=(shape(images.shape, BF16), shape((n_tiles, 16, LANES), BF16), shape((8, LANES), F32)),
            in_specs=[aspec] * 8,
            out_specs=(aspec, vspec, vspec),
            scratch_shapes=scratch,
            compiler_params=pltpu.CompilerParams(
                collective_id=0, has_side_effects=True, vmem_limit_bytes=65000000
            ),
        )(
            images, out_grad, conv_weight, proj_weight, gain_one.reshape(1, C), shift_one.reshape(1, C),
            gain_three.reshape(nb3, LANES), shift_three.reshape(nb3, LANES),
        )
        got = pl.pallas_call(
            finish,
            out_shape=(
                shape(images.shape, BF16), shape((3, 3, C, C), F32), shape((C, CO), F32), shape((1, C), F32),
                shape((1, C), F32), shape((nb3, LANES), F32), shape((nb3, LANES), F32),
            ),
            in_specs=[aspec] * 3,
            out_specs=(aspec,) + (vspec,) * 6,
            scratch_shapes=[
                vm((C, TH, W), BF16), vm((n_tiles, 16, LANES), BF16), vm((8, LANES), F32), pltpu.SemaphoreType.DMA((10,))
            ],
            compiler_params=pltpu.CompilerParams(vmem_limit_bytes=65000000),
        )(img, tiles, sums)
        return (
            got[0], got[1], got[2], got[3].reshape(C), got[4].reshape(C), got[5].reshape(CO), got[6].reshape(CO),
        )

    split = P(("bn", "dp"), "sp", None, None, None)
    return jax.shard_map(
        step,
        mesh=mesh,
        in_specs=(split, split) + (P(),) * 6,
        out_specs=(split,) + (P(),) * 6,
        check_vma=False,
    )
```

```python
import functools

import jax
import jax.numpy as jnp
from jax import lax
from jax.experimental import pallas as pl
from jax.experimental.pallas import tpu as pltpu
from jax.sharding import PartitionSpec as P

MESH = pl.DeviceIdType.MESH
F32 = jnp.float32
BF16 = jnp.bfloat16
EPS = 1e-05
LANES = 128


def dot(a, b):
    return lax.dot_general(a, b, (((1,), (0,)), ((), ())), preferred_element_type=F32)


def dot_nt(a, b):
    return lax.dot_general(a, b, (((1,), (1,)), ((), ())), preferred_element_type=F32)


def to_column(row):
    return jnp.transpose(jnp.broadcast_to(row, (LANES, LANES)))


def columns_of(rows, depth):
    parts = [to_column(rows[k : k + 1]) for k in range(rows.shape[0])]
    return jnp.concatenate(parts, axis=0)[:depth] if len(parts) > 1 else parts[0][:depth]


def put_rows(ref, first, second):
    depth = first.shape[0]
    blocks = ref.shape[0] // 2
    lane = lax.broadcasted_iota(jnp.int32, (depth, LANES), 1)
    table = jnp.where(lane == 0, first, jnp.where(lane == 1, second, 0.0))
    if depth < LANES:
        table = jnp.concatenate([table, jnp.zeros((LANES - depth, LANES), F32)], axis=0)
    for k in range(blocks):
        turned = jnp.transpose(table[k * LANES : (k + 1) * LANES])
        ref[k : k + 1, :] = turned[0:1]
        ref[blocks + k : blocks + k + 1, :] = turned[1:2]


def kernel(
    n_sp, n_bn, n_dp, per_image,
    img, cot, cw_in, pw_in, g1_in, b1_in, g3_in, b3_in,
    o_img, o_agr, o_sums,
    xin, gin, flat, gflat, xs, hid, slope, ybuf, wide, egrad, das, out,
    wfwd, wbwd, wproj, col_s, col_r, row_r, diag_r, row_s, dcol_s, dcol_r, drow_s, drow_r, ddiag_r,
    m1s, m1r, m3s, m3r, q3s, q3r, q1s, q1r, dw, pg, tiles, rtiles, dts, dtr, vs, vr, ags, agr, vec,
    co3, co1, dh, htiles, rhtiles, gram, ebuf,
    cw, pw, g1, b1, g3, b3, rsem, ssem, lsem,
):
    C, TH, W = xin.shape
    CO = gin.shape[0]
    NG = n_sp * n_bn
    nb1, nb3 = m1s.shape[0] // 2, m3s.shape[0] // 2
    n_local = float(TH * W)
    M = n_local * NG
    sp, bn, dp = lax.axis_index("sp"), lax.axis_index("bn"), lax.axis_index("dp")
    me = sp * n_bn + bn
    column = lax.rem(sp, 2)
    rowhalf = sp // 2

    def wrapped(at, step, size):
        moved = at + step
        return jnp.where(moved >= size, moved - size, moved)

    xs_of = [wrapped(sp, k, n_sp) for k in range(n_sp)]
    zs_of = [wrapped(bn, k, n_bn) for k in range(n_bn)]
    ds_of = [wrapped(dp, k, n_dp) for k in range(n_dp)]

    def ring(step, size):
        return min(step, size - step)

    peers = sorted(range(1, NG), key=lambda k: -ring(k // n_bn, n_sp) - ring(k % n_bn, n_bn))
    others = sorted(range(1, n_dp), key=lambda k: -ring(k // 2, n_dp // 2))

    def peer(k):
        return (xs_of[k // n_bn], zs_of[k % n_bn], dp)

    def across(k):
        return (sp, bn, ds_of[k])

    in_x = pltpu.make_async_copy(img.at[0, 0], xin, lsem.at[0])
    in_g = pltpu.make_async_copy(cot.at[0, 0], gin, lsem.at[1])
    pairs = ((cw_in, cw), (pw_in, pw), (g1_in, g1), (b1_in, b1), (g3_in, g3), (b3_in, b3))
    small = [pltpu.make_async_copy(src, dst, lsem.at[3 + i]) for i, (src, dst) in enumerate(pairs)]
    in_x.start()
    for copy in small:
        copy.start()
    in_g.start()

    barrier = pltpu.get_barrier_semaphore()

    for k in peers:
        pl.semaphore_signal(barrier, inc=1, device_id=peer(k), device_id_type=MESH)
    for k in others:
        pl.semaphore_signal(barrier, inc=1, device_id=across(k), device_id_type=MESH)

    for copy in small:
        copy.wait()
    taps = [cw[n // 3, n % 3].astype(F32) for n in range(9)]
    wfwd[...] = jnp.concatenate(taps, axis=1).astype(BF16)
    flipped = jnp.concatenate([taps[8 - n] for n in range(9)], axis=0)
    wbwd[...] = jnp.transpose(flipped).astype(BF16)
    wproj[...] = jnp.transpose(pw[...].astype(F32)).astype(BF16)
    vec[...] = jnp.zeros_like(vec)
    vec[0:1, 0:C] = g1[...]
    vec[1:2, 0:C] = b1[...]
    vec[2 : 2 + nb3, :] = g3[...]
    vec[2 + nb3 : 2 + 2 * nb3, :] = b3[...]

    in_x.wait()

    def widen(c, carry):
        flat[pl.ds(pl.multiple_of(c * TH, 8), TH), :] = xin[c].astype(F32)
        return carry

    lax.fori_loop(0, C, widen, 0, unroll=4)

    lane = lax.broadcasted_iota(jnp.int32, (C, W), 1)
    edge_mine = jnp.where(column == 0, W - 1, 0)
    edge_other = (W - 1) - edge_mine
    row_mine = jnp.where(rowhalf == 0, TH - 1, 0)
    halo_row = jnp.where(rowhalf == 0, TH + 1, 0)
    empty_row = (TH + 1) - halo_row

    def pick(h):
        return flat[pl.ds(h, C, stride=TH), :]

    def gather_column(row_of):
        def step(h, packed):
            turned = pltpu.roll(row_of(h), lax.rem(h - edge_mine + W, W), 1)
            return jnp.where(lane == h, turned, packed)

        return lax.fori_loop(0, TH, step, jnp.zeros((C, W), F32), unroll=4)

    col_s[...] = gather_column(pick).astype(BF16)
    row_s[...] = pick(row_mine).astype(BF16)

    def build(dst, h, row):
        left = jnp.where(lane == 0, 0.0, pltpu.roll(row, 1, 1))
        right = jnp.where(lane == W - 1, 0.0, pltpu.roll(row, W - 1, 1))
        dst[h + 1, 0:C, :] = left.astype(BF16)
        dst[h + 1, C : 2 * C, :] = row.astype(BF16)
        dst[h + 1, 2 * C : 3 * C, :] = right.astype(BF16)

    def lay_out(h, carry):
        build(xs, h, pick(h))
        return carry

    lax.fori_loop(0, TH, lay_out, 0, unroll=4)
    xs[empty_row] = jnp.zeros((3 * C, W), BF16)

    pl.semaphore_wait(barrier, NG - 1 + n_dp - 1)

    beside = (sp + 1 - 2 * column, bn, dp)
    below = (lax.rem(sp + 2, 4), bn, dp)
    corner = (3 - sp, bn, dp)

    def halo(cs, cr, rs, rr, dr, base):
        return [
            pltpu.make_async_remote_copy(cs, cr, ssem.at[base], rsem.at[base], device_id=beside, device_id_type=MESH),
            pltpu.make_async_remote_copy(
                rs, rr, ssem.at[base + 1], rsem.at[base + 1], device_id=below, device_id_type=MESH
            ),
            pltpu.make_async_remote_copy(
                rs, dr, ssem.at[base + 2], rsem.at[base + 2], device_id=corner, device_id_type=MESH
            ),
        ]

    x_halo = halo(col_s, col_r, row_s, row_r, diag_r, 0)
    for copy in x_halo:
        copy.start()

    in_g.wait()

    def widen_g(c, carry):
        gflat[pl.ds(pl.multiple_of(c * TH, 8), TH), :] = gin[c].astype(F32)
        return carry

    lax.fori_loop(0, CO, widen_g, 0, unroll=8)

    inner = pl.ds(pl.multiple_of(jnp.where(column == 0, 2 * C, 0), 16), C)

    def patch(dst, cr, rr, dr):
        sides = cr[...].astype(F32)

        def step(h, carry):
            side = pltpu.roll(sides, lax.rem(edge_mine - h + W, W), 1)
            dst[h + 1, inner, :] = jnp.where(lane == edge_mine, side, dst[h + 1, inner, :].astype(F32)).astype(BF16)
            return carry

        lax.fori_loop(0, TH, step, 0, unroll=4)
        build(dst, halo_row - 1, rr[...].astype(F32))
        side = pltpu.roll(dr[...].astype(F32), lax.rem(edge_mine - edge_other + W, W), 1)
        held = dst[halo_row, inner, :].astype(F32)
        dst[halo_row, inner, :] = jnp.where(lane == edge_mine, side, held).astype(BF16)

    for copy in x_halo:
        copy.wait()
    patch(xs, col_r, row_r, diag_r)

    R = 4

    def stack(src, h):
        parts = [src[pl.ds(h + j, 3)].reshape(9 * C, W) for j in range(R)]
        return jnp.concatenate(parts, axis=1)

    def conv(p, carry):
        h = p * R
        block = dot(wfwd[...], stack(xs, h))
        for j in range(R):
            hid[h + j] = block[:, j * W : (j + 1) * W]
        return carry

    lax.fori_loop(0, TH // R, conv, 0)

    def exchange(src, dst, n):
        pltpu.make_async_copy(src, dst.at[me], rsem.at[n]).start()

        for k in peers:
            pltpu.make_async_remote_copy(
                src, dst.at[me], ssem.at[n], rsem.at[n], device_id=peer(k), device_id_type=MESH
            ).start()

    def arrived(dst, n):
        pltpu.make_async_copy(dst, dst, rsem.at[n]).wait()

    def moments(src, depth, message):
        chunk = min(depth, 64)
        firsts, seconds = [], []
        for c in range(0, depth, chunk):
            base = jnp.sum(src[0, c : c + chunk, :], axis=1, keepdims=True) * (1.0 / W)
            shift = jnp.broadcast_to(base, (chunk, W))

            def step(p, carry):
                total, squares = carry
                for j in range(4):
                    v = src[p * 4 + j, c : c + chunk, :] - shift
                    total = total + v
                    squares = squares + v * v
                return total, squares

            zero = jnp.zeros((chunk, W), F32)
            total, squares = lax.fori_loop(0, TH // 4, step, (zero, zero))
            local = jnp.sum(total, axis=1, keepdims=True)
            firsts.append(base + local * (1.0 / n_local))
            seconds.append(jnp.sum(squares, axis=1, keepdims=True) - local * local * (1.0 / n_local))
        put_rows(message, jnp.concatenate(firsts, axis=0), jnp.concatenate(seconds, axis=0))

    def combined(ref, blocks):
        means = ref[:, 0:blocks, :]
        mean = jnp.sum(means, axis=0) * (1.0 / NG)
        off = means - mean[None]
        total = jnp.sum(ref[:, blocks : 2 * blocks, :], axis=0) + n_local * jnp.sum(off * off, axis=0)
        return mean, lax.rsqrt(total * (1.0 / M) + EPS)

    moments(hid, C, m1s)
    exchange(m1s, m1r, 6)

    def lay_out_g(h, carry):
        for c in range(0, CO, 32):
            egrad[h, c : c + 32, :] = gflat[pl.ds(c * TH + h, 32, stride=TH), :]
        return carry

    lax.fori_loop(0, TH, lay_out_g, 0)
    arrived(m1r, 6)
    mean1, scale1 = combined(m1r, nb1)
    gain1, bias1 = vec[0:1, :], vec[1:2, :]
    co1[0] = columns_of(0.5 * gain1 * scale1, C)
    co1[1] = columns_of(0.5 * (bias1 - mean1 * gain1 * scale1), C)
    middle = jnp.floor(bias1 * (8.0 + 8.0 * jnp.tanh(0.5 * bias1)) + 0.5) * (1.0 / 16.0)
    co1[2] = columns_of(middle, C)
    gram[...] = jnp.zeros_like(gram)

    def activate(p, carry):
        h = p * R
        rows = []
        for j in range(R):
            half = hid[h + j] * co1[0] + co1[1]
            t = jnp.tanh(half)
            u = 1.0 + t
            y = (half * u).astype(BF16)
            hid[h + j] = half
            slope[h + j] = 0.5 * u * (1.0 + half * (1.0 - t))
            ybuf[h + j] = y
            rows.append((y.astype(F32) - co1[2]).astype(BF16))
        off = jnp.concatenate(rows, axis=1)
        gram[...] += dot_nt(jnp.concatenate([off, jnp.ones((16, R * W), BF16)], axis=0), off)
        return carry

    lax.fori_loop(0, TH // R, activate, 0)
    gram[C : C + 8, :] = gram[C : C + 8, :] * (1.0 / n_local)
    gram[C + 8 : C + 16, :] = jnp.broadcast_to(middle[:, 0:C], (8, C))
    table = gram[...]
    high = table.astype(BF16)
    rest = table - high.astype(F32)
    mid = rest.astype(BF16)
    low = (rest - mid.astype(F32)).astype(BF16)
    turned = dot(jnp.concatenate([high, mid, low], axis=0), pw[...])
    turned = turned[0 : C + 16] + turned[C + 16 : 2 * C + 32] + turned[2 * C + 32 :]
    local = turned[C : C + 1]
    spread_of = jnp.sum(turned[0:C] * pw[...].astype(F32), axis=0, keepdims=True) - n_local * local * local
    local = local + turned[C + 8 : C + 9]
    for k in range(nb3):
        m3s[k : k + 1, :] = local[:, k * LANES : (k + 1) * LANES]
        m3s[nb3 + k : nb3 + k + 1, :] = spread_of[:, k * LANES : (k + 1) * LANES]
    exchange(m3s, m3r, 7)

    def project(p, carry):
        h = p * R
        block = dot(wproj[...], jnp.concatenate([ybuf[h + j] for j in range(R)], axis=1))
        for j in range(R):
            wide[h + j] = block[:, j * W : (j + 1) * W]
        return carry

    lax.fori_loop(0, TH // R, project, 0)

    lt_c = dw.shape[1] // LANES
    lt_p = CO // LANES
    n_conv = C // 16 * lt_c
    n_tiles = n_conv + C // 16 * lt_p

    def scatter(src, dst, low, high, n):
        def send(to):
            owner = to[0] * n_bn + to[1]

            @pl.when(jnp.logical_and(owner >= low, owner < high))
            def _():
                pltpu.make_async_remote_copy(
                    src.at[owner], dst.at[me], ssem.at[n], rsem.at[n], device_id=to, device_id_type=MESH
                ).start()

        @pl.when(jnp.logical_and(me >= low, me < high))
        def _():
            pltpu.make_async_copy(src.at[me], dst.at[me], rsem.at[n]).start()

        for k in peers:
            send(peer(k))

    dh[...] = jnp.zeros_like(dh)

    def weigh(p, carry):
        h = p * R
        ones = jnp.ones((16, W), BF16)
        rows = [jnp.concatenate([hid[h + j].astype(BF16), ones], axis=0) for j in range(R)]
        dh[:, 0 : 9 * C] += dot_nt(jnp.concatenate(rows, axis=1), stack(xs, h))
        return carry

    lax.fori_loop(0, TH // R, weigh, 0)
    for r in range(C // 16):
        for t in range(lt_c):
            cols = slice(t * LANES, (t + 1) * LANES)
            htiles[r * lt_c + t, 0:16, :] = dh[r * 16 : (r + 1) * 16, cols]
            htiles[r * lt_c + t, 16:24, :] = dh[C : C + 8, cols]
    scatter(htiles, rhtiles, 0, n_conv, 14)

    arrived(m3r, 7)
    mean3, scale3 = combined(m3r, nb3)
    gain3, bias3 = vec[2 : 2 + nb3, :], vec[2 + nb3 : 2 + 2 * nb3, :]
    co3[0] = columns_of(0.5 * gain3 * scale3, CO)
    co3[1] = columns_of(0.5 * (bias3 - mean3 * gain3 * scale3), CO)

    step_c = 32
    firsts, seconds = [], []
    for c in range(0, CO, step_c):
        alpha, beta = co3[0, c : c + step_c, :], co3[1, c : c + step_c, :]

        def slopes(p, carry):
            total, cross = carry
            for j in range(8):
                h = p * 8 + j
                half = wide[h, c : c + step_c, :] * alpha + beta
                t = jnp.tanh(half)
                g = egrad[h, c : c + step_c, :]
                e = g * ((1.0 + t) * (1.0 + half * (1.0 - t)))
                wide[h, c : c + step_c, :] = half
                egrad[h, c : c + step_c, :] = e
                total = total + e
                cross = cross + e * half
            return total, cross

        zero = jnp.zeros((step_c, W), F32)
        total, cross = lax.fori_loop(0, TH // 8, slopes, (zero, zero))
        firsts.append(jnp.sum(total, axis=1, keepdims=True))
        seconds.append(jnp.sum(cross, axis=1, keepdims=True))
    put_rows(q3s, jnp.concatenate(firsts, axis=0), jnp.concatenate(seconds, axis=0))
    exchange(q3s, q3r, 8)
    arrived(q3r, 8)
    e_sum = jnp.sum(q3r[:, 0:nb3, :], axis=0)
    eh_sum = jnp.sum(q3r[:, nb3 : 2 * nb3, :], axis=0)
    s3 = 0.5 * e_sum
    q3 = (eh_sum - bias3 * s3) / gain3
    vs[...] = jnp.zeros_like(vs)
    vs[0:nb3, :] = s3
    vs[nb3 : 2 * nb3, :] = q3
    co3[1] = columns_of((-2.0 / M) * scale3 * q3, CO)
    co3[2] = columns_of((1.0 / M) * scale3 * (q3 * bias3 - gain3 * s3), CO)

    pg[...] = jnp.zeros_like(pg)
    dw[...] = jnp.zeros_like(dw)
    ebuf[...] = jnp.zeros_like(ebuf)

    def max_of(p):
        return jnp.where(p < 0, 0, p)

    def unproject(p, carry):
        total, cross = carry
        h = p * R
        pieces = []
        for c in range(0, CO, 32):
            part = slice(c, c + 32)
            alpha, beta, gamma = co3[0, part, :], co3[1, part, :], co3[2, part, :]
            rows = [
                (egrad[h + j, part, :] * alpha + wide[h + j, part, :] * beta + gamma).astype(BF16) for j in range(R)
            ]
            pieces.append(jnp.concatenate(rows, axis=1))
        grads = jnp.concatenate(pieces, axis=0)
        hidden = jnp.concatenate([ybuf[h + j] for j in range(R)], axis=1)
        pg[...] += dot_nt(hidden, grads)
        block = dot(pw[...], grads)
        held = max_of(p - 1) * R
        dw[:, 0 : 9 * C] += dot_nt(ebuf[...], stack(xs, held))
        rows = []
        for j in range(R):
            e = block[:, j * W : (j + 1) * W] * slope[h + j]
            slope[h + j] = e
            rows.append(e.astype(BF16))
            total = total + e
            cross = cross + e * hid[h + j]
        ebuf[...] = jnp.concatenate(rows, axis=1)
        return total, cross

    zero = jnp.zeros((C, W), F32)
    total, cross = lax.fori_loop(0, TH // R, unproject, (zero, zero))
    dw[:, 0 : 9 * C] += dot_nt(ebuf[...], stack(xs, TH - R))

    for r in range(C // 16):
        rows = slice(r * 16, (r + 1) * 16)
        for t in range(lt_c):
            tiles[r * lt_c + t] = dw[rows, t * LANES : (t + 1) * LANES]
        for t in range(lt_p):
            tiles[n_conv + r * lt_p + t] = pg[rows, t * LANES : (t + 1) * LANES]
    put_rows(q1s, jnp.sum(total, axis=1, keepdims=True), jnp.sum(cross, axis=1, keepdims=True))
    exchange(q1s, q1r, 9)
    scatter(tiles, rtiles, 0, n_tiles, 10)

    arrived(q1r, 9)
    s1 = jnp.sum(q1r[:, 0:nb1, :], axis=0)
    eh1 = jnp.sum(q1r[:, nb1 : 2 * nb1, :], axis=0)
    safe = jnp.where(lax.broadcasted_iota(jnp.int32, (1, LANES), 1) < C, gain1, 1.0)
    q1 = (2.0 * eh1 - bias1 * s1) / safe
    vs[2 * nb3 : 2 * nb3 + 1, :] = s1
    vs[2 * nb3 + 1 : 2 * nb3 + 2, :] = q1
    co1[0] = columns_of(gain1 * scale1, C)
    co1[1] = columns_of((-2.0 / M) * scale1 * q1, C)
    co1[2] = columns_of((1.0 / M) * scale1 * (q1 * bias1 - gain1 * s1), C)

    def spread(src, dst, n):
        pltpu.make_async_copy(src, dst.at[dp], rsem.at[n]).start()

        for k in others:
            pltpu.make_async_remote_copy(
                src, dst.at[dp], ssem.at[n], rsem.at[n], device_id=across(k), device_id_type=MESH
            ).start()

    spread(vs, vr, 11)

    def unnorm(h, packed):
        row = slope[h] * co1[0] + hid[h] * co1[1] + co1[2]
        slope[h] = row
        build(das, h, row)
        turned = pltpu.roll(row, lax.rem(h - edge_mine + W, W), 1)
        return jnp.where(lane == h, turned, packed)

    dcol_s[...] = lax.fori_loop(0, TH, unnorm, jnp.zeros((C, W), F32), unroll=4).astype(BF16)
    drow_s[...] = slope[row_mine].astype(BF16)
    d_halo = halo(dcol_s, dcol_r, drow_s, drow_r, ddiag_r, 3)
    for copy in d_halo:
        copy.start()

    das[empty_row] = jnp.zeros((3 * C, W), BF16)

    @pl.when(me < n_conv)
    def _():
        arrived(rhtiles, 14)
        arrived(rtiles, 10)
        rows = pl.ds(pl.multiple_of((me // lt_c) * 16, 16), 16)
        whole = jnp.sum(rtiles[...], axis=0) * co1[0, rows, :]
        whole = whole + jnp.sum(rhtiles[:, 0:16, :], axis=0) * co1[1, rows, :]
        whole = whole + jnp.sum(rhtiles[:, 16:17, :], axis=0) * co1[2, rows, :]
        dts[...] = whole.astype(BF16)

    @pl.when(jnp.logical_and(me >= n_conv, me < n_tiles))
    def _():
        arrived(rtiles, 10)
        dts[...] = jnp.sum(rtiles[...], axis=0).astype(BF16)

    @pl.when(me < n_tiles)
    def _():
        spread(dts, dtr, 12)

    for copy in d_halo:
        copy.wait()
    patch(das, dcol_r, drow_r, ddiag_r)

    def unconv(p, carry):
        h = p * R
        block = dot(wbwd[...], stack(das, h))
        for j in range(R):
            flat[pl.ds(h + j, C, stride=TH), :] = block[:, j * W : (j + 1) * W]
        return carry

    lax.fori_loop(0, TH // R, unconv, 0)

    def narrow(c, carry):
        out[c] = flat[pl.ds(pl.multiple_of(c * TH, 8), TH), :].astype(BF16)
        return carry

    lax.fori_loop(0, C, narrow, 0, unroll=4)
    put = pltpu.make_async_copy(out, o_img.at[0, 0], lsem.at[2])
    put.start()

    @pl.when(me < n_tiles)
    def _():
        arrived(dtr, 12)
        ags[...] = (jnp.sum(dtr[...].astype(F32), axis=0) * per_image).astype(BF16)
        exchange(ags, agr, 13)

    arrived(vr, 11)
    o_sums[...] = jnp.sum(vr[...], axis=0) * per_image

    gathered = agr.at[pl.ds(0, n_tiles)]
    pltpu.make_async_copy(gathered, gathered, rsem.at[13]).wait()
    o_agr[...] = agr[0:n_tiles]

    for dst, n in ((m1r, 6), (m3r, 7), (q3r, 8), (q1r, 9)):
        sent = dst.at[pl.ds(0, NG - 1)]
        pltpu.make_async_copy(sent, sent, ssem.at[n]).wait()
    sent = vr.at[pl.ds(0, n_dp - 1)]
    pltpu.make_async_copy(sent, sent, ssem.at[11]).wait()

    @pl.when(me < n_tiles)
    def _():
        sent = rtiles.at[pl.ds(0, n_tiles - 1)]
        pltpu.make_async_copy(sent, sent, ssem.at[10]).wait()
        sent = dtr.at[pl.ds(0, n_dp - 1)]
        pltpu.make_async_copy(sent, sent, ssem.at[12]).wait()
        sent = agr.at[pl.ds(0, NG - 1)]
        pltpu.make_async_copy(sent, sent, ssem.at[13]).wait()

    @pl.when(me >= n_tiles)
    def _():
        sent = rtiles.at[pl.ds(0, n_tiles)]
        pltpu.make_async_copy(sent, sent, ssem.at[10]).wait()

    @pl.when(me < n_conv)
    def _():
        sent = rhtiles.at[pl.ds(0, n_conv - 1)]
        pltpu.make_async_copy(sent, sent, ssem.at[14]).wait()

    @pl.when(me >= n_conv)
    def _():
        sent = rhtiles.at[pl.ds(0, n_conv)]
        pltpu.make_async_copy(sent, sent, ssem.at[14]).wait()

    put.wait()


def finish(img, agr_in, sums_in, o_img, o_cw, o_pw, o_g1, o_b1, o_g3, o_b3, held, agr, sums, sem):
    small = [pltpu.make_async_copy(agr_in, agr, sem.at[0]), pltpu.make_async_copy(sums_in, sums, sem.at[1])]
    parts = 4
    step = held.shape[0] // parts
    cuts = [pl.ds(k * step, step) for k in range(parts)]
    come = [pltpu.make_async_copy(img.at[0, 0, c], held.at[c], sem.at[2 + k]) for k, c in enumerate(cuts)]
    leave = [pltpu.make_async_copy(held.at[c], o_img.at[0, 0, c], sem.at[2 + parts + k]) for k, c in enumerate(cuts)]
    for copy in small + come:
        copy.start()
    for there, back in zip(come, leave):
        there.wait()
        back.start()
    for copy in small:
        copy.wait()
    C = o_pw.shape[0]
    nb3 = o_g3.shape[0]
    lt_p = o_pw.shape[1] // LANES
    lt_c = -(-9 * C // LANES)
    n_conv = C // 16 * lt_c
    o_b3[...] = sums[0:nb3]
    o_g3[...] = sums[nb3 : 2 * nb3]
    o_b1[...] = sums[2 * nb3 : 2 * nb3 + 1, 0:C]
    o_g1[...] = sums[2 * nb3 + 1 : 2 * nb3 + 2, 0:C]
    for r in range(C // 16):
        rows = slice(r * 16, (r + 1) * 16)
        for t in range(lt_p):
            o_pw[rows, t * LANES : (t + 1) * LANES] = agr[n_conv + r * lt_p + t].astype(F32)
        line = [agr[r * lt_c + t].astype(F32) for t in range(lt_c)]
        line = jnp.concatenate(line, axis=1)
        for n in range(9):
            o_cw[n // 3, n % 3, rows, :] = line[:, n * C : (n + 1) * C]
    for copy in leave:
        copy.wait()


def solution(mesh):
    n_sp, n_bn, n_dp = mesh.shape["sp"], mesh.shape["bn"], mesh.shape["dp"]
    NG = n_sp * n_bn

    def step(images, out_grad, conv_weight, proj_weight, gain_one, shift_one, gain_three, shift_three):
        C, TH, W = images.shape[2:]
        CO = out_grad.shape[2]
        nb1, nb3 = 1, CO // LANES
        wide_c = -(-9 * C // LANES) * LANES
        n_conv = C // 16 * (wide_c // LANES)
        n_tiles = n_conv + C // 16 * (CO // LANES)
        vm = pltpu.VMEM
        scratch = [
            vm((C, TH, W), BF16), vm((CO, TH, W), BF16), vm((C * TH, W), F32), vm((CO * TH, W), F32),
            vm((TH + 2, 3 * C, W), BF16), vm((TH, C, W), F32), vm((TH, C, W), F32), vm((TH, C, W), BF16),
            vm((TH, CO, W), F32), vm((TH, CO, W), F32), vm((TH + 2, 3 * C, W), BF16), vm((C, TH, W), BF16),
            vm((C, 9 * C), BF16), vm((C, 9 * C), BF16), vm((CO, C), BF16),
            *[vm((C, W), BF16) for _ in range(10)][:5], *[vm((C, W), BF16) for _ in range(5)],
            vm((2 * nb1, LANES), F32), vm((NG, 2 * nb1, LANES), F32),
            vm((2 * nb3, LANES), F32), vm((NG, 2 * nb3, LANES), F32),
            vm((2 * nb3, LANES), F32), vm((NG, 2 * nb3, LANES), F32),
            vm((2 * nb1, LANES), F32), vm((NG, 2 * nb1, LANES), F32),
            vm((C, wide_c), F32), vm((C, CO), F32), vm((n_tiles, 16, LANES), F32), vm((NG, 16, LANES), F32),
            vm((16, LANES), BF16), vm((n_dp, 16, LANES), BF16), vm((8, LANES), F32), vm((n_dp, 8, LANES), F32),
            vm((16, LANES), BF16), vm((NG, 16, LANES), BF16), vm((8, LANES), F32),
            vm((3, CO, W), F32), vm((3, C, W), F32),
            vm((C + 16, wide_c), F32), vm((n_conv, 24, LANES), F32), vm((NG, 24, LANES), F32), vm((C + 16, C), F32), vm((C, 4 * W), BF16),
            vm((3, 3, C, C), BF16), vm((C, CO), BF16), vm((1, C), F32), vm((1, C), F32), vm((nb3, LANES), F32),
            vm((nb3, LANES), F32),
            pltpu.SemaphoreType.DMA((15,)), pltpu.SemaphoreType.DMA((15,)), pltpu.SemaphoreType.DMA((9,)),
        ]
        vspec = pl.BlockSpec(memory_space=pltpu.VMEM)
        aspec = pl.BlockSpec(memory_space=pl.ANY)
        shape = jax.ShapeDtypeStruct
        img, tiles, sums = pl.pallas_call(
            functools.partial(kernel, n_sp, n_bn, n_dp, 1.0 / float(n_sp * TH * W)),
            out_shape=(shape(images.shape, BF16), shape((n_tiles, 16, LANES), BF16), shape((8, LANES), F32)),
            in_specs=[aspec] * 8,
            out_specs=(aspec, vspec, vspec),
            scratch_shapes=scratch,
            compiler_params=pltpu.CompilerParams(
                collective_id=0, has_side_effects=True, vmem_limit_bytes=65000000
            ),
        )(
            images, out_grad, conv_weight, proj_weight, gain_one.reshape(1, C), shift_one.reshape(1, C),
            gain_three.reshape(nb3, LANES), shift_three.reshape(nb3, LANES),
        )
        got = pl.pallas_call(
            finish,
            out_shape=(
                shape(images.shape, BF16), shape((3, 3, C, C), F32), shape((C, CO), F32), shape((1, C), F32),
                shape((1, C), F32), shape((nb3, LANES), F32), shape((nb3, LANES), F32),
            ),
            in_specs=[aspec] * 3,
            out_specs=(aspec,) + (vspec,) * 6,
            scratch_shapes=[
                vm((C, TH, W), BF16), vm((n_tiles, 16, LANES), BF16), vm((8, LANES), F32), pltpu.SemaphoreType.DMA((10,))
            ],
            compiler_params=pltpu.CompilerParams(vmem_limit_bytes=65000000),
        )(img, tiles, sums)
        return (
            got[0], got[1], got[2], got[3].reshape(C), got[4].reshape(C), got[5].reshape(CO), got[6].reshape(CO),
        )

    split = P(("bn", "dp"), "sp", None, None, None)
    return jax.shard_map(
        step,
        mesh=mesh,
        in_specs=(split, split) + (P(),) * 6,
        out_specs=(split,) + (P(),) * 6,
        check_vma=False,
    )
```
